512 devices in a mesh: energy: 2 (over y), slab: 16 (over z), orb: 8 (over x), rhs: 2 (over core).
Axes of the slice: x: 8, y: 2, z: 16, core: 2. Of those that a mesh axis runs over, the one named last changes fastest.
The devices are a block of a 8x8x16 slice.
Arguments:
- diag_blocks: float32 [64, 192, 384], P(('energy', 'slab'), 'orb'), parts along dimension 0, may hold values from -8 to 8, as said below
- couplings: float32 [64, 192, 384], P(('energy', 'slab')), parts along dimension 0, may hold values from -8 to 8
- sources: float32 [64, 128, 384], P(('energy', 'slab'), ('orb', 'rhs')), parts along dimension 0, may hold values from -8 to 8
Outputs:
- solution: float32 [64, 128, 384], P(('energy', 'slab'), ('orb', 'rhs')), parts along dimension 0
The draws below stay inside these ranges and needn't reach their ends.
There are 2 independent parts, one for each index of `energy`. The reference program is written for one: setup_inputs(seed, part) draws one part's arguments, and reference() takes and returns one part's arrays. A program takes and returns all parts, laid end to end along the dimension named above; each array names one. Nothing has to cross between parts.
Inputs may be any that keep to these rules, and one draw needn't show every extreme that they name: Every diag_blocks[n] is Hermitian, and together with couplings it makes K positive definite with smallest eigenvalue 0.01 or more.
All inputs are finite; a program needn't handle non-finite values.
Results may differ from the reference program's by a relative error of at most 0.0003.
Values sent between devices are 32-bit elements; how exact they have to be, the bound alone decides.
No kernel may reach another device: no remote copies, remote signals or barrier semaphores. Data moves between devices by JAX's collectives and lax.ppermute only.
A program may use at most 128 MiB of HBM per device.

```python
import math
import jax
import jax.numpy as jnp
from jax import lax

NO = 192
NL = 32
NRHS = 128


def layer_matrices(key):
    base = jax.random.fold_in(key, 1723)
    keys = jax.random.split(base, 6)
    spread = 0.5 / math.sqrt(2.0 * NO)
    identity = jnp.eye(NO, dtype=jnp.float32)
    left_real = identity + spread * jax.random.normal(keys[0], (NL, NO, NO), jnp.float32)
    left_imag = spread * jax.random.normal(keys[1], (NL, NO, NO), jnp.float32)
    right_real = identity + spread * jax.random.normal(keys[2], (NL, NO, NO), jnp.float32)
    right_imag = spread * jax.random.normal(keys[3], (NL, NO, NO), jnp.float32)
    level_shift = jnp.exp(jax.random.uniform(keys[4], (), jnp.float32, math.log(0.01), math.log(0.03)))
    shifts = level_shift * jnp.exp(jax.random.uniform(keys[5], (NL,), jnp.float32, 0.0, math.log(4.0)))
    return (left_real, left_imag, right_real, right_imag, shifts)


def hermitian_product(first_real, first_imag, second_real, second_imag):
    real_part = jnp.einsum('nki,nkj->nij', first_real, second_real) + jnp.einsum('nki,nkj->nij', first_imag, second_imag)
    imag_part = jnp.einsum('nki,nkj->nij', first_real, second_imag) - jnp.einsum('nki,nkj->nij', first_imag, second_real)
    return (real_part, imag_part)


def column_major(real_part, imag_part):
    return jnp.concatenate([jnp.swapaxes(real_part, 1, 2), jnp.swapaxes(imag_part, 1, 2)], axis=2)


def draw_diag_blocks(key, part):
    left_real, left_imag, right_real, right_imag, shifts = layer_matrices(key)
    own_real, own_imag = hermitian_product(right_real, right_imag, right_real, right_imag)
    next_real, next_imag = hermitian_product(left_real, left_imag, left_real, left_imag)
    has_above = (jnp.arange(NL) >= 1).astype(jnp.float32)[:, None, None]
    padding = jnp.zeros((1, NO, NO), jnp.float32)
    below_real = jnp.concatenate([next_real[1:], padding], axis=0)
    below_imag = jnp.concatenate([next_imag[1:], padding], axis=0)
    identity = jnp.eye(NO, dtype=jnp.float32)
    real_part = has_above * own_real + below_real + shifts[:, None, None] * identity
    imag_part = has_above * own_imag + below_imag
    return column_major(real_part, imag_part)


def draw_couplings(key, part):
    left_real, left_imag, right_real, right_imag, shifts = layer_matrices(key)
    cross_real, cross_imag = hermitian_product(right_real, right_imag, left_real, left_imag)
    has_above = (jnp.arange(NL) >= 1).astype(jnp.float32)[:, None, None]
    return column_major(-has_above * cross_real, -has_above * cross_imag)


def draw_sources(key, part):
    base = jax.random.fold_in(key, 3301)
    keys = jax.random.split(base, 1)
    return jnp.clip(jax.random.normal(keys[0], (NL, NRHS, 2 * NO), jnp.float32), -6.0, 6.0)


def setup_inputs(seed: int = 0, part: int = 0) -> dict:
    seeds = jax.random.split(jax.random.key(seed), 4)
    own_keys = jax.random.split(jax.random.fold_in(seeds[3], part), 4)
    return {
        "diag_blocks": draw_diag_blocks(jax.random.fold_in(jax.random.fold_in(seeds[3], part), 71), part),
        "couplings": draw_couplings(jax.random.fold_in(jax.random.fold_in(seeds[3], part), 71), part),
        "sources": draw_sources(jax.random.fold_in(jax.random.fold_in(seeds[3], part), 71), part),
    }


def embed(columns):
    block_order = columns.shape[-1] // 2
    turned = jnp.concatenate([-columns[..., block_order:], columns[..., :block_order]], axis=-1)
    return jnp.concatenate([columns, turned], axis=-2)

def times(left, right):
    return jnp.dot(left.astype(jnp.float32), right.astype(jnp.float32), precision=lax.Precision.HIGHEST, preferred_element_type=jnp.float32)

def times_flipped(left, right):
    return lax.dot_general(left.astype(jnp.float32), right.astype(jnp.float32), (((1,), (1,)), ((), ())), precision=lax.Precision.HIGHEST, preferred_element_type=jnp.float32)

def apply_inverse(factor, rows):
    return jax.scipy.linalg.cho_solve((factor, True), rows.T).T

def reference(diag_blocks, couplings, sources):
    layer_count = diag_blocks.shape[0]
    block_order = diag_blocks.shape[2] // 2
    keep = (jnp.arange(layer_count) > 0).astype(couplings.dtype)
    couplings = couplings * keep[:, None, None]
    embedded = jax.vmap(embed)(couplings)

    def forward(carry, item):
        factor_prev, load_prev = carry
        block, coupling_embed, source = item
        herm_block = coupling_embed[:, :block_order].T
        pivot = block - times(apply_inverse(factor_prev, herm_block), coupling_embed)
        load = source - times(apply_inverse(factor_prev, load_prev), coupling_embed)
        factor = jnp.linalg.cholesky(embed(pivot))
        return ((factor, load), (factor, load))
    start_factor = jnp.eye(2 * block_order, dtype=diag_blocks.dtype)
    start_load = jnp.zeros_like(sources[0])
    _, (factors, loads) = lax.scan(forward, (start_factor, start_load), (diag_blocks, embedded, sources))
    next_embeds = jnp.concatenate([embedded[1:], jnp.zeros_like(embedded[:1])], axis=0)

    def backward(upper_value, item):
        factor, load, next_embed = item
        value = apply_inverse(factor, load - times_flipped(upper_value, next_embed))
        return (value, value)
    _, solution = lax.scan(backward, jnp.zeros_like(sources[0]), (factors, loads, next_embeds), reverse=True)
    return solution
```

```python
import functools
import jax
import jax.numpy as jnp
from jax import lax
from jax.experimental import pallas as pl
from jax.experimental.pallas import tpu as pltpu
from jax.sharding import PartitionSpec as P


HI = lax.Precision.HIGHEST
LANES = 128
HALF = 64
SUB = 8


def mm(a, b):
    return lax.dot_general(a, b, (((1,), (0,)), ((), ())), precision=HI, preferred_element_type=jnp.float32)


def mm_t(a, b):
    return lax.dot_general(a, b, (((1,), (1,)), ((), ())), precision=HI, preferred_element_type=jnp.float32)


def lanes_of(x):
    return lax.broadcasted_iota(jnp.int32, x.shape, 1)


def times_i(x):
    parts = []
    for b in range(x.shape[1] // LANES):
        blk = x[:, b * LANES : (b + 1) * LANES]
        rolled = pltpu.roll(blk, HALF, 1)
        parts.append(jnp.where(lanes_of(blk) < HALF, -rolled, rolled))
    return jnp.concatenate(parts, axis=1)


def embed(z):
    rows = []
    turned = times_i(z)
    for a in range(z.shape[0] // HALF):
        rows.append(z[a * HALF : (a + 1) * HALF])
        rows.append(turned[a * HALF : (a + 1) * HALF])
    return jnp.concatenate(rows, axis=0)


def first_rows(e):
    return jnp.concatenate([e[a * LANES : a * LANES + HALF] for a in range(e.shape[0] // LANES)], axis=0)


def blocked(x):
    v0, v1, v2 = (x[:, LANES * b : LANES * (b + 1)] for b in range(3))
    low = lanes_of(v0) < HALF
    return jnp.concatenate(
        [jnp.where(low, v0, v1), pltpu.roll(jnp.where(low, v2, v0), HALF, 1), jnp.where(low, v1, v2)], axis=1
    )


def unblocked(x):
    u0, u1, u2 = (x[:, LANES * b : LANES * (b + 1)] for b in range(3))
    low = lanes_of(u0) < HALF
    r1 = pltpu.roll(u1, HALF, 1)
    return jnp.concatenate([jnp.where(low, u0, r1), jnp.where(low, u2, u0), jnp.where(low, r1, u2)], axis=1)


def pairs(n):
    return [(a, b) for a in range(n) for b in range(a, n)]


def packed(z):
    n = z.shape[0] // HALF
    return jnp.concatenate(
        [z[a * HALF : (a + 1) * HALF, b * LANES : (b + 1) * LANES] for a, b in pairs(n)], axis=0
    )


def adjoint(block):
    t = block.T
    return jnp.concatenate([t[:HALF], -t[HALF:]], axis=1)


def unpack_to(ref, p):
    n = ref.shape[0] // HALF
    for k, (a, b) in enumerate(pairs(n)):
        block = p[k * HALF : (k + 1) * HALF]
        ref[a * HALF : (a + 1) * HALF, b * LANES : (b + 1) * LANES] = block
        if a != b:
            ref[b * HALF : (b + 1) * HALF, a * LANES : (a + 1) * LANES] = adjoint(block)


def lane_copy(x, lane):
    return jnp.broadcast_to(x[:, lane : lane + 1], (SUB, LANES))


def row_copy(x, row):
    return jnp.broadcast_to(x[row : row + 1, :], (SUB, LANES))


def invert(m_ref):
    order = m_ref.shape[0]
    nb = order // HALF
    groups = HALF // SUB
    lane = lax.broadcasted_iota(jnp.int32, (SUB, LANES), 1)
    sub = lax.broadcasted_iota(jnp.int32, (SUB, LANES), 0)
    low = lane < HALF
    lane_in = jnp.where(low, lane, lane - HALF)
    zero = jnp.zeros((SUB, LANES), jnp.float32)
    for k in range(nb):
        x = [
            [m_ref[k * HALF + g * SUB : k * HALF + (g + 1) * SUB, b * LANES : (b + 1) * LANES] for b in range(nb)]
            for g in range(groups)
        ]
        for t in range(groups):
            z = list(x[t])
            y = []
            for b in range(nb):
                rolled = pltpu.roll(z[b], HALF, 1)
                y.append(jnp.where(low, -rolled, rolled))
            vr = [lane_copy(z[k], SUB * t + j) for j in range(SUB)]
            vi = [lane_copy(z[k], HALF + SUB * t + j) for j in range(SUB)]
            for p in range(SUB):
                here = sub == p
                col = lane_in == SUB * t + p
                rinv = 1.0 / row_copy(vr[p], p)
                fr = jnp.where(here, -rinv, vr[p] * rinv)
                fi = jnp.where(here, 0.0, vi[p] * rinv)
                for j in range(p + 1, SUB):
                    ar, ai = row_copy(vr[j], p), row_copy(vi[j], p)
                    vr[j] = jnp.where(here, 0.0, vr[j]) - (fr * ar - fi * ai)
                    vi[j] = jnp.where(here, 0.0, vi[j]) - (fr * ai + fi * ar)
                for b in range(nb):
                    zr, yr = row_copy(z[b], p), row_copy(y[b], p)
                    base_z, base_y = jnp.where(here, 0.0, z[b]), jnp.where(here, 0.0, y[b])
                    if b == k:
                        zr = jnp.where(col, jnp.where(low, 1.0, 0.0), zr)
                        yr = jnp.where(col, jnp.where(low, 0.0, 1.0), yr)
                        base_z, base_y = jnp.where(col, 0.0, base_z), jnp.where(col, 0.0, base_y)
                    z[b] = base_z - (fr * zr + fi * yr)
                    y[b] = base_y - (fr * yr - fi * zr)
            x[t] = z
            cols = (lane_in >= SUB * t) & (lane_in < SUB * (t + 1))
            order_g = [(t + 1 + s) % groups for s in range(groups - 1)]
            lr = {g: [lane_copy(x[g][k], SUB * t + j) for j in range(SUB)] for g in order_g}
            li = {g: [lane_copy(x[g][k], HALF + SUB * t + j) for j in range(SUB)] for g in order_g}
            zs = [[row_copy(z[b], j) for b in range(nb)] for j in range(SUB)]
            ys = [[row_copy(y[b], j) for b in range(nb)] for j in range(SUB)]
            for g in order_g:
                new = []
                for b in range(nb):
                    base = jnp.where(cols, 0.0, x[g][b]) if b == k else x[g][b]
                    acc = [lr[g][j] * zs[j][b] + li[g][j] * ys[j][b] for j in range(SUB)]
                    while len(acc) > 1:
                        acc = [acc[i] + acc[i + 1] for i in range(0, len(acc), 2)]
                    new.append(base - acc[0])
                x[g] = new
        for g in range(groups):
            for b in range(nb):
                m_ref[k * HALF + g * SUB : k * HALF + (g + 1) * SUB, b * LANES : (b + 1) * LANES] = x[g][b]
        zr = m_ref[k * HALF : (k + 1) * HALF, :]
        right = jnp.concatenate([zr, times_i(zr)], axis=0)
        others = [a for a in range(nb) if a != k]
        left = jnp.concatenate(
            [m_ref[a * HALF : (a + 1) * HALF, k * LANES : (k + 1) * LANES] for a in others], axis=0
        )
        change = mm(left, right)
        for i, a in enumerate(others):
            for b in range(nb):
                piece = change[i * HALF : (i + 1) * HALF, b * LANES : (b + 1) * LANES]
                sl = (slice(a * HALF, (a + 1) * HALF), slice(b * LANES, (b + 1) * LANES))
                m_ref[sl] = -piece if b == k else m_ref[sl] - piece


def joined(blocks):
    return jnp.concatenate(blocks, axis=0)


def lane_blocks(z):
    return joined([z[:, b * LANES : (b + 1) * LANES] for b in range(z.shape[1] // LANES)])


def from_lane_blocks(ref, start, rows, count):
    return jnp.concatenate([ref[start + b * rows : start + (b + 1) * rows, :] for b in range(count)], axis=1)


def start_kernel(diag_ref, coup_ref, w_ref, t_ref, vv_ref):
    w_ref[...] = blocked(diag_ref[0])
    invert(w_ref)
    second = embed(blocked(coup_ref[1]))
    t = mm(first_rows(second.T), embed(w_ref[...]))
    t_ref[...] = t
    vv_ref[...] = packed(blocked(diag_ref[1]) - mm(t, second))


def start_side_kernel(slab_ref, coup_ref, src_ref, w_ref, t_ref, send_ref, load_ref, wl_ref, back_ref):
    order = w_ref.shape[0]
    cols = src_ref.shape[1]
    count = w_ref.shape[1] // LANES
    keep = (slab_ref[0] > 0).astype(jnp.float32)
    first = blocked(coup_ref[0]) * keep
    first_e = embed(first)
    t = t_ref[...]
    own = mm(joined([first, blocked(src_ref[0])]), embed(w_ref[...]))
    t2, wl = own[:order], own[order:]
    change = mm_t(joined([t, t2, wl]), first_e)
    gu = -change[2 * order :]
    gv = blocked(src_ref[1]) - mm(wl, embed(blocked(coup_ref[1])))
    load = joined([gu, gv])
    load_ref[...] = load
    send_ref[...] = joined(
        [lane_blocks(-change[:order]), packed(-change[order : 2 * order]), lane_blocks(load)]
    )
    wl_ref[...] = wl
    back_ref[...] = joined([embed(t2), embed(t)])


def merge_kernel(theirs_ref, vv_ref, send_ref, w_ref, t_ref, new_vv_ref):
    order = w_ref.shape[0]
    count = w_ref.shape[1] // LANES
    size = vv_ref.shape[0]
    unpack_to(w_ref, theirs_ref[...] + send_ref[count * order : count * order + size, :])
    invert(w_ref)
    second = from_lane_blocks(send_ref, 0, order, count)
    t = mm(second, embed(w_ref[...]))
    t_ref[...] = t
    new_vv_ref[...] = vv_ref[...] - packed(mm_t(t, embed(second)))


def side_kernel(w_ref, t_ref, mine_ref, theirs_ref, send_ref, load_ref, wl_ref, back_ref):
    order = w_ref.shape[0]
    count = w_ref.shape[1] // LANES
    rest = count * order
    cols = load_ref.shape[0] // 2
    size = send_ref.shape[0] - rest - count * 2 * cols
    first_e = embed(from_lane_blocks(theirs_ref, 0, order, count))
    second_e = embed(from_lane_blocks(mine_ref, 0, order, count))
    my_load = from_lane_blocks(mine_ref, rest + size, 2 * cols, count)
    their_load = from_lane_blocks(theirs_ref, rest + size, 2 * cols, count)
    t = t_ref[...]
    own = mm(joined([first_rows(first_e.T), their_load[cols:] + my_load[:cols]]), embed(w_ref[...]))
    t2, wl = own[:order], own[order:]
    change = mm(joined([t, t2, wl]), first_e)
    gu = their_load[:cols] - change[2 * order :]
    gv = my_load[cols:] - mm_t(wl, second_e)
    load = joined([gu, gv])
    load_ref[...] = load
    send_ref[...] = joined(
        [
            lane_blocks(-change[:order]),
            theirs_ref[rest : rest + size, :] - packed(change[order : 2 * order]),
            lane_blocks(load),
        ]
    )
    wl_ref[...] = wl
    back_ref[...] = joined([embed(t2), embed(t)])


def last_kernel(theirs_ref, mine_ref, w_ref, t_ref, vv_ref, send_ref, out_ref, vl_ref, m_ref):
    order = w_ref.shape[0]
    count = w_ref.shape[1] // LANES
    cols = theirs_ref.shape[0] // 2
    unpack_to(m_ref, vv_ref[...])
    invert(m_ref)
    second_e = embed(from_lane_blocks(send_ref, 0, order, count))
    wl = mm(theirs_ref[cols:, :] + mine_ref[:cols, :], embed(w_ref[...]))
    gv = mine_ref[cols:, :] - mm_t(wl, second_e)
    vl = mm(gv, embed(m_ref[...]))
    mid = wl - mm(vl, embed(t_ref[...]))
    out_ref[...] = joined([jnp.zeros_like(mid), mid])
    vl_ref[...] = vl


def values_of(level, slab_ref, got_ref, prev_ref, vl_ref, wl_ref, back_ref):
    cols = wl_ref.shape[0]
    span = 2 << level
    aimed = lax.rem(slab_ref[0], span) == (span // 2 - 1)
    vu = jnp.where(aimed, got_ref[:cols, :], prev_ref[cols:, :])
    vl = jnp.where(aimed, got_ref[cols:, :], vl_ref[...])
    mid = wl_ref[...] - mm(jnp.concatenate([vu, vl], axis=1), back_ref[...])
    return vu, mid, vl


def back_kernel(level, slab_ref, got_ref, prev_ref, vl_ref, wl_ref, back_ref, out_ref, new_vl_ref):
    vu, mid, vl = values_of(level, slab_ref, got_ref, prev_ref, vl_ref, wl_ref, back_ref)
    out_ref[...] = joined([vu, mid])
    new_vl_ref[...] = vl


def end_kernel(slab_ref, got_ref, prev_ref, vl_ref, wl_ref, back_ref, out_ref):
    _, mid, vl = values_of(0, slab_ref, got_ref, prev_ref, vl_ref, wl_ref, back_ref)
    out_ref[0] = unblocked(mid)
    out_ref[1] = unblocked(vl)


def f32(*shape):
    return jax.ShapeDtypeStruct(shape, jnp.float32)


def run(kernel, outs, *args, scalars=0, flops=10**8, scratch=()):
    specs = [pl.BlockSpec(memory_space=pltpu.SMEM)] * scalars
    specs += [pl.BlockSpec(memory_space=pltpu.VMEM)] * (len(args) - scalars)
    return pl.pallas_call(
        kernel,
        out_shape=outs,
        in_specs=specs,
        out_specs=jax.tree.map(lambda _: pl.BlockSpec(memory_space=pltpu.VMEM), outs),
        scratch_shapes=list(scratch),
        cost_estimate=pl.CostEstimate(flops=flops, bytes_accessed=10**6, transcendentals=0),
    )(*args)


def forward_to(x, axis, distance):
    n = lax.axis_size(axis)
    pairs_ = [(i, i + distance) for i in range(distance - 1, n, 2 * distance)]
    return lax.ppermute(x, axis, pairs_)


def back_to(x, axis, distance):
    n = lax.axis_size(axis)
    pairs_ = [(i + distance, i) for i in range(distance - 1, n, 2 * distance)]
    return lax.ppermute(x, axis, pairs_)


def gathered(diag_blocks):
    layer = diag_blocks[0]
    other = diag_blocks[1]
    mine = jnp.where(lax.axis_index("rhs") == 0, layer, other)
    copies = jnp.broadcast_to(mine, (lax.axis_size("orb"), *mine.shape))
    whole = lax.all_to_all(copies, "orb", split_axis=0, concat_axis=0, tiled=True)
    return lax.all_gather(whole.reshape(-1, mine.shape[1]), "rhs")


def local(diag_blocks, couplings, sources):
    order, width = couplings.shape[1:]
    cols = sources.shape[1]
    nb = order // HALF
    size = len(pairs(nb)) * HALF
    whole = f32(order, width)
    vv_shape = f32(size, LANES)
    sides = (
        f32((order + 2 * cols) * width // LANES + size, LANES),
        f32(2 * cols, width),
        f32(cols, width),
        f32(4 * order, width),
    )
    slab = lax.axis_index("slab").astype(jnp.int32).reshape(1)
    heavy, light = 4 * 10**9, 10**9
    w, t, vv = run(start_kernel, (whole, whole, vv_shape), gathered(diag_blocks), couplings, flops=heavy)
    levels = lax.axis_size("slab").bit_length() - 1
    stored = []
    send = load = None
    for level in range(levels):
        their_vv = forward_to(vv, "slab", 1 << level)
        if level == 0:
            send, load, wl, back = run(
                start_side_kernel, sides, slab, couplings, sources, w, t, scalars=1, flops=light
            )
        else:
            send, load, wl, back = run(side_kernel, sides, w, t, send, theirs, flops=light)
        stored.append((wl, back))
        if level < levels - 1:
            theirs = forward_to(send, "slab", 1 << level)
        else:
            theirs = forward_to(load, "slab", 1 << level)
        w, t, vv = run(merge_kernel, (whole, whole, vv_shape), their_vv, vv, send, flops=heavy)
    pair = f32(2 * cols, width)
    values, vl = run(
        last_kernel,
        (pair, f32(cols, width)),
        theirs,
        load,
        w,
        t,
        vv,
        send,
        flops=heavy,
        scratch=[pltpu.VMEM((order, width), jnp.float32)],
    )
    for level in reversed(range(levels)):
        got = back_to(values, "slab", 1 << level)
        wl, back = stored[level]
        if level > 0:
            values, vl = run(
                functools.partial(back_kernel, level),
                (pair, f32(cols, width)),
                slab, got, values, vl, wl, back,
                scalars=1, flops=10**7,
            )
    return run(end_kernel, f32(2, cols, width), slab, got, values, vl, wl, back, scalars=1, flops=10**7)


def solution(mesh):
    placed = (
        P(("energy", "slab"), "orb", None),
        P(("energy", "slab"), None, None),
        P(("energy", "slab"), ("orb", "rhs"), None),
    )
    return jax.shard_map(
        local,
        mesh=mesh,
        in_specs=placed,
        out_specs=P(("energy", "slab"), ("orb", "rhs"), None),
        check_vma=False,
    )
```

```python
import functools
import jax
import jax.numpy as jnp
from jax import lax
from jax.experimental import pallas as pl
from jax.experimental.pallas import tpu as pltpu
from jax.sharding import PartitionSpec as P


HI = lax.Precision.HIGHEST
LANES = 128
HALF = 64
SUB = 8
LIMIT = 16 * 2**20


def mm(a, b):
    return lax.dot_general(a, b, (((1,), (0,)), ((), ())), precision=HI, preferred_element_type=jnp.float32)


def mm_t(a, b):
    return lax.dot_general(a, b, (((1,), (1,)), ((), ())), precision=HI, preferred_element_type=jnp.float32)


def lanes_of(x):
    return lax.broadcasted_iota(jnp.int32, x.shape, 1)


def times_i(x):
    parts = []
    for b in range(x.shape[1] // LANES):
        blk = x[:, b * LANES : (b + 1) * LANES]
        rolled = pltpu.roll(blk, HALF, 1)
        parts.append(jnp.where(lanes_of(blk) < HALF, -rolled, rolled))
    return jnp.concatenate(parts, axis=1)


def embed(z):
    rows = []
    turned = times_i(z)
    for a in range(z.shape[0] // HALF):
        rows.append(z[a * HALF : (a + 1) * HALF])
        rows.append(turned[a * HALF : (a + 1) * HALF])
    return jnp.concatenate(rows, axis=0)


def first_rows(e):
    return jnp.concatenate([e[a * LANES : a * LANES + HALF] for a in range(e.shape[0] // LANES)], axis=0)


def blocked(x):
    v0, v1, v2 = (x[:, LANES * b : LANES * (b + 1)] for b in range(3))
    low = lanes_of(v0) < HALF
    return jnp.concatenate(
        [jnp.where(low, v0, v1), pltpu.roll(jnp.where(low, v2, v0), HALF, 1), jnp.where(low, v1, v2)], axis=1
    )


def unblocked(x):
    u0, u1, u2 = (x[:, LANES * b : LANES * (b + 1)] for b in range(3))
    low = lanes_of(u0) < HALF
    r1 = pltpu.roll(u1, HALF, 1)
    return jnp.concatenate([jnp.where(low, u0, r1), jnp.where(low, u2, u0), jnp.where(low, r1, u2)], axis=1)


def pairs(n):
    return [(a, b) for a in range(n) for b in range(a, n)]


def packed(z):
    n = z.shape[0] // HALF
    return jnp.concatenate(
        [z[a * HALF : (a + 1) * HALF, b * LANES : (b + 1) * LANES] for a, b in pairs(n)], axis=0
    )


def adjoint(block):
    t = block.T
    return jnp.concatenate([t[:HALF], -t[HALF:]], axis=1)


def unpack_to(ref, p):
    n = ref.shape[0] // HALF
    for k, (a, b) in enumerate(pairs(n)):
        block = p[k * HALF : (k + 1) * HALF]
        ref[a * HALF : (a + 1) * HALF, b * LANES : (b + 1) * LANES] = block
        if a != b:
            ref[b * HALF : (b + 1) * HALF, a * LANES : (a + 1) * LANES] = adjoint(block)


def lane_copy(x, lane):
    return jnp.broadcast_to(x[:, lane : lane + 1], (SUB, LANES))


def row_copy(x, row):
    return jnp.broadcast_to(x[row : row + 1, :], (SUB, LANES))


def invert(m_ref):
    order = m_ref.shape[0]
    nb = order // HALF
    groups = HALF // SUB
    lane = lax.broadcasted_iota(jnp.int32, (SUB, LANES), 1)
    sub = lax.broadcasted_iota(jnp.int32, (SUB, LANES), 0)
    low = lane < HALF
    lane_in = jnp.where(low, lane, lane - HALF)
    zero = jnp.zeros((SUB, LANES), jnp.float32)
    for k in range(nb):
        x = [
            [m_ref[k * HALF + g * SUB : k * HALF + (g + 1) * SUB, b * LANES : (b + 1) * LANES] for b in range(nb)]
            for g in range(groups)
        ]
        for t in range(groups):
            z = list(x[t])
            y = []
            for b in range(nb):
                rolled = pltpu.roll(z[b], HALF, 1)
                y.append(jnp.where(low, -rolled, rolled))
            vr = [lane_copy(z[k], SUB * t + j) for j in range(SUB)]
            vi = [lane_copy(z[k], HALF + SUB * t + j) for j in range(SUB)]
            for p in range(SUB):
                here = sub == p
                col = lane_in == SUB * t + p
                rinv = 1.0 / row_copy(vr[p], p)
                fr = jnp.where(here, -rinv, vr[p] * rinv)
                fi = jnp.where(here, 0.0, vi[p] * rinv)
                for j in range(p + 1, SUB):
                    ar, ai = row_copy(vr[j], p), row_copy(vi[j], p)
                    vr[j] = jnp.where(here, 0.0, vr[j]) - (fr * ar - fi * ai)
                    vi[j] = jnp.where(here, 0.0, vi[j]) - (fr * ai + fi * ar)
                for b in range(nb):
                    zr, yr = row_copy(z[b], p), row_copy(y[b], p)
                    base_z, base_y = jnp.where(here, 0.0, z[b]), jnp.where(here, 0.0, y[b])
                    if b == k:
                        zr = jnp.where(col, jnp.where(low, 1.0, 0.0), zr)
                        yr = jnp.where(col, jnp.where(low, 0.0, 1.0), yr)
                        base_z, base_y = jnp.where(col, 0.0, base_z), jnp.where(col, 0.0, base_y)
                    z[b] = base_z - (fr * zr + fi * yr)
                    y[b] = base_y - (fr * yr - fi * zr)
            x[t] = z
            cols = (lane_in >= SUB * t) & (lane_in < SUB * (t + 1))
            order_g = [(t + 1 + s) % groups for s in range(groups - 1)]
            lr = {g: [lane_copy(x[g][k], SUB * t + j) for j in range(SUB)] for g in order_g}
            li = {g: [lane_copy(x[g][k], HALF + SUB * t + j) for j in range(SUB)] for g in order_g}
            zs = [[row_copy(z[b], j) for b in range(nb)] for j in range(SUB)]
            ys = [[row_copy(y[b], j) for b in range(nb)] for j in range(SUB)]
            for g in order_g:
                new = []
                for b in range(nb):
                    base = jnp.where(cols, 0.0, x[g][b]) if b == k else x[g][b]
                    acc = [lr[g][j] * zs[j][b] + li[g][j] * ys[j][b] for j in range(SUB)]
                    while len(acc) > 1:
                        acc = [acc[i] + acc[i + 1] for i in range(0, len(acc), 2)]
                    new.append(base - acc[0])
                x[g] = new
        for g in range(groups):
            for b in range(nb):
                m_ref[k * HALF + g * SUB : k * HALF + (g + 1) * SUB, b * LANES : (b + 1) * LANES] = x[g][b]
        zr = m_ref[k * HALF : (k + 1) * HALF, :]
        right = jnp.concatenate([zr, times_i(zr)], axis=0)
        others = [a for a in range(nb) if a != k]
        left = jnp.concatenate(
            [m_ref[a * HALF : (a + 1) * HALF, k * LANES : (k + 1) * LANES] for a in others], axis=0
        )
        change = mm(left, right)
        for i, a in enumerate(others):
            for b in range(nb):
                piece = change[i * HALF : (i + 1) * HALF, b * LANES : (b + 1) * LANES]
                sl = (slice(a * HALF, (a + 1) * HALF), slice(b * LANES, (b + 1) * LANES))
                m_ref[sl] = -piece if b == k else m_ref[sl] - piece


def rows_times(x, z):
    blocks = [x[:, b * LANES : (b + 1) * LANES] for b in range(x.shape[1] // LANES)]
    low = lanes_of(blocks[0]) < HALF
    turned = [pltpu.roll(b, HALF, 1) for b in blocks]
    even = range(0, len(blocks) - 1, 2)
    re = [jnp.where(low, blocks[b], turned[b + 1]) for b in even]
    im = [jnp.where(low, turned[b], blocks[b + 1]) for b in even]
    if len(blocks) % 2:
        re.append(blocks[-1][:, :HALF])
        im.append(turned[-1][:, :HALF])
    both = jnp.concatenate([jnp.concatenate(re, axis=1), jnp.concatenate(im, axis=1)], axis=0)
    got = mm(both, z)
    n = x.shape[0]
    return got[:n] + times_i(got[n:])


def joined(blocks):
    return jnp.concatenate(blocks, axis=0)


def lane_blocks(z):
    return joined([z[:, b * LANES : (b + 1) * LANES] for b in range(z.shape[1] // LANES)])


def from_lane_blocks(ref, start, rows, count):
    return jnp.concatenate([ref[start + b * rows : start + (b + 1) * rows, :] for b in range(count)], axis=1)


def start_kernel(diag_ref, coup_ref, w_ref, t_ref, vv_ref):
    w_ref[...] = blocked(diag_ref[1])
    invert(w_ref)
    second = blocked(coup_ref[1])
    t = mm(second, embed(w_ref[...]))
    t_ref[...] = t
    vv_ref[...] = packed(blocked(diag_ref[0]) - mm_t(t, embed(second)))


def start_side_kernel(coup_ref, next_ref, src_ref, w_ref, t_ref, send_ref, load_ref, wl_ref, back_ref):
    order = w_ref.shape[0]
    first_e = embed(blocked(next_ref[...]))
    t = t_ref[...]
    own = mm(joined([first_rows(first_e.T), blocked(src_ref[1])]), embed(w_ref[...]))
    t2, wl = own[:order], own[order:]
    change = mm(joined([t, t2, wl]), first_e)
    gu = -change[2 * order :]
    gv = blocked(src_ref[0]) - mm_t(wl, embed(blocked(coup_ref[1])))
    load = joined([gu, gv])
    load_ref[...] = load
    send_ref[...] = joined(
        [lane_blocks(-change[:order]), packed(-change[order : 2 * order]), lane_blocks(load)]
    )
    wl_ref[...] = wl
    back_ref[...] = joined([t2, t])


def merge_kernel(theirs_ref, vv_ref, send_ref, w_ref, t_ref, new_vv_ref):
    order = w_ref.shape[0]
    count = w_ref.shape[1] // LANES
    size = vv_ref.shape[0]
    unpack_to(w_ref, theirs_ref[...] + send_ref[count * order : count * order + size, :])
    invert(w_ref)
    second = from_lane_blocks(send_ref, 0, order, count)
    t = mm(second, embed(w_ref[...]))
    t_ref[...] = t
    new_vv_ref[...] = vv_ref[...] - packed(mm_t(t, embed(second)))


def side_kernel(w_ref, t_ref, mine_ref, theirs_ref, send_ref, load_ref, wl_ref, back_ref):
    order = w_ref.shape[0]
    count = w_ref.shape[1] // LANES
    rest = count * order
    cols = load_ref.shape[0] // 2
    size = send_ref.shape[0] - rest - count * 2 * cols
    first_e = embed(from_lane_blocks(theirs_ref, 0, order, count))
    second_e = embed(from_lane_blocks(mine_ref, 0, order, count))
    my_load = from_lane_blocks(mine_ref, rest + size, 2 * cols, count)
    their_load = from_lane_blocks(theirs_ref, rest + size, 2 * cols, count)
    t = t_ref[...]
    own = mm(joined([first_rows(first_e.T), their_load[cols:] + my_load[:cols]]), embed(w_ref[...]))
    t2, wl = own[:order], own[order:]
    change = mm(joined([t, t2, wl]), first_e)
    gu = their_load[:cols] - change[2 * order :]
    gv = my_load[cols:] - mm_t(wl, second_e)
    load = joined([gu, gv])
    load_ref[...] = load
    send_ref[...] = joined(
        [
            lane_blocks(-change[:order]),
            theirs_ref[rest : rest + size, :] - packed(change[order : 2 * order]),
            lane_blocks(load),
        ]
    )
    wl_ref[...] = wl
    back_ref[...] = joined([t2, t])


def last_kernel(theirs_ref, mine_ref, w_ref, t_ref, vv_ref, send_ref, out_ref, vl_ref, m_ref):
    order = w_ref.shape[0]
    count = w_ref.shape[1] // LANES
    cols = theirs_ref.shape[0] // 2
    unpack_to(m_ref, vv_ref[...])
    invert(m_ref)
    second_e = embed(from_lane_blocks(send_ref, 0, order, count))
    wl = rows_times(theirs_ref[cols:, :] + mine_ref[:cols, :], w_ref[...])
    gv = mine_ref[cols:, :] - mm_t(wl, second_e)
    vl = rows_times(gv, m_ref[...])
    mid = wl - rows_times(vl, t_ref[...])
    out_ref[...] = joined([jnp.zeros_like(mid), mid])
    vl_ref[...] = vl


def values_of(level, slab_ref, got_ref, prev_ref, vl_ref, wl_ref, back_ref):
    cols = wl_ref.shape[0]
    span = 2 << level
    aimed = lax.rem(slab_ref[0], span) == span // 2
    vu = jnp.where(aimed, got_ref[:cols, :], prev_ref[cols:, :])
    vl = jnp.where(aimed, got_ref[cols:, :], vl_ref[...])
    mid = wl_ref[...] - rows_times(jnp.concatenate([vu, vl], axis=1), back_ref[...])
    return vu, mid, vl


def back_kernel(level, slab_ref, got_ref, prev_ref, vl_ref, wl_ref, back_ref, out_ref, new_vl_ref):
    vu, mid, vl = values_of(level, slab_ref, got_ref, prev_ref, vl_ref, wl_ref, back_ref)
    out_ref[...] = joined([vu, mid])
    new_vl_ref[...] = vl


def end_kernel(slab_ref, got_ref, prev_ref, vl_ref, wl_ref, back_ref, out_ref):
    _, mid, vl = values_of(0, slab_ref, got_ref, prev_ref, vl_ref, wl_ref, back_ref)
    out_ref[0] = unblocked(vl)
    out_ref[1] = unblocked(mid)


def f32(*shape):
    return jax.ShapeDtypeStruct(shape, jnp.float32)


def run(kernel, outs, *args, scalars=0, flops=10**8, scratch=()):
    specs = [pl.BlockSpec(memory_space=pltpu.SMEM)] * scalars
    specs += [pl.BlockSpec(memory_space=pltpu.VMEM)] * (len(args) - scalars)
    return pl.pallas_call(
        kernel,
        out_shape=outs,
        in_specs=specs,
        out_specs=jax.tree.map(lambda _: pl.BlockSpec(memory_space=pltpu.VMEM), outs),
        scratch_shapes=list(scratch),
        compiler_params=pltpu.CompilerParams(vmem_limit_bytes=LIMIT),
        cost_estimate=pl.CostEstimate(flops=flops, bytes_accessed=10**6, transcendentals=0),
    )(*args)


def forward_to(x, axis, distance):
    n = lax.axis_size(axis)
    return lax.ppermute(x, axis, [(i + distance, i) for i in range(0, n, 2 * distance)])


def back_to(x, axis, distance):
    n = lax.axis_size(axis)
    return lax.ppermute(x, axis, [(i, i + distance) for i in range(0, n, 2 * distance)])


def gathered(diag_blocks):
    layer = diag_blocks[0]
    other = diag_blocks[1]
    mine = jnp.where(lax.axis_index("rhs") == 0, layer, other)
    copies = jnp.broadcast_to(mine, (lax.axis_size("orb"), *mine.shape))
    whole = lax.all_to_all(copies, "orb", split_axis=0, concat_axis=0, tiled=True)
    return lax.all_gather(whole.reshape(-1, mine.shape[1]), "rhs")


def local(diag_blocks, couplings, sources):
    order, width = couplings.shape[1:]
    cols = sources.shape[1]
    nb = order // HALF
    size = len(pairs(nb)) * HALF
    whole = f32(order, width)
    vv_shape = f32(size, LANES)
    sides = (
        f32((order + 2 * cols) * width // LANES + size, LANES),
        f32(2 * cols, width),
        f32(cols, width),
        f32(2 * order, width),
    )
    slab = lax.axis_index("slab").astype(jnp.int32).reshape(1)
    heavy, light = 4 * 10**9, 10**9
    n = lax.axis_size("slab")
    following = lax.ppermute(couplings[0], "slab", [(i + 1, i) for i in range(n - 1)])
    w, t, vv = run(start_kernel, (whole, whole, vv_shape), gathered(diag_blocks), couplings, flops=heavy)
    levels = lax.axis_size("slab").bit_length() - 1
    stored = []
    send = load = None
    for level in range(levels):
        their_vv = forward_to(vv, "slab", 1 << level)
        if level == 0:
            send, load, wl, back = run(
                start_side_kernel, sides, couplings, following, sources, w, t, flops=light
            )
        else:
            send, load, wl, back = run(side_kernel, sides, w, t, send, theirs, flops=light)
        stored.append((wl, back))
        if level < levels - 1:
            theirs = forward_to(send, "slab", 1 << level)
        else:
            theirs = forward_to(load, "slab", 1 << level)
        w, t, vv = run(merge_kernel, (whole, whole, vv_shape), their_vv, vv, send, flops=heavy)
    pair = f32(2 * cols, width)
    values, vl = run(
        last_kernel,
        (pair, f32(cols, width)),
        theirs,
        load,
        w,
        t,
        vv,
        send,
        flops=heavy,
        scratch=[pltpu.VMEM((order, width), jnp.float32)],
    )
    for level in reversed(range(levels)):
        got = back_to(values, "slab", 1 << level)
        wl, back = stored[level]
        if level > 0:
            values, vl = run(
                functools.partial(back_kernel, level),
                (pair, f32(cols, width)),
                slab, got, values, vl, wl, back,
                scalars=1, flops=10**7,
            )
    return run(end_kernel, f32(2, cols, width), slab, got, values, vl, wl, back, scalars=1, flops=10**7)


def solution(mesh):
    placed = (
        P(("energy", "slab"), "orb", None),
        P(("energy", "slab"), None, None),
        P(("energy", "slab"), ("orb", "rhs"), None),
    )
    return jax.shard_map(
        local,
        mesh=mesh,
        in_specs=placed,
        out_specs=P(("energy", "slab"), ("orb", "rhs"), None),
        check_vma=False,
    )
```

```python
import functools
import jax
import jax.numpy as jnp
from jax import lax
from jax.experimental import pallas as pl
from jax.experimental.pallas import tpu as pltpu
from jax.sharding import PartitionSpec as P


HI = lax.Precision.HIGHEST
LANES = 128
HALF = 64
SUB = 8
LIMIT = 16 * 2**20


def mm(a, b):
    return lax.dot_general(a, b, (((1,), (0,)), ((), ())), precision=HI, preferred_element_type=jnp.float32)


def mm_t(a, b):
    return lax.dot_general(a, b, (((1,), (1,)), ((), ())), precision=HI, preferred_element_type=jnp.float32)


def lanes_of(x):
    return lax.broadcasted_iota(jnp.int32, x.shape, 1)


def times_i(x):
    parts = []
    for b in range(x.shape[1] // LANES):
        blk = x[:, b * LANES : (b + 1) * LANES]
        rolled = pltpu.roll(blk, HALF, 1)
        parts.append(jnp.where(lanes_of(blk) < HALF, -rolled, rolled))
    return jnp.concatenate(parts, axis=1)


def embed(z):
    rows = []
    turned = times_i(z)
    for a in range(z.shape[0] // HALF):
        rows.append(z[a * HALF : (a + 1) * HALF])
        rows.append(turned[a * HALF : (a + 1) * HALF])
    return jnp.concatenate(rows, axis=0)


def first_rows(e):
    return jnp.concatenate([e[a * LANES : a * LANES + HALF] for a in range(e.shape[0] // LANES)], axis=0)


def blocked(x):
    v0, v1, v2 = (x[:, LANES * b : LANES * (b + 1)] for b in range(3))
    low = lanes_of(v0) < HALF
    return jnp.concatenate(
        [jnp.where(low, v0, v1), pltpu.roll(jnp.where(low, v2, v0), HALF, 1), jnp.where(low, v1, v2)], axis=1
    )


def unblocked(x):
    u0, u1, u2 = (x[:, LANES * b : LANES * (b + 1)] for b in range(3))
    low = lanes_of(u0) < HALF
    r1 = pltpu.roll(u1, HALF, 1)
    return jnp.concatenate([jnp.where(low, u0, r1), jnp.where(low, u2, u0), jnp.where(low, r1, u2)], axis=1)


def pairs(n):
    return [(a, b) for a in range(n) for b in range(a, n)]


def packed(z):
    n = z.shape[0] // HALF
    return jnp.concatenate(
        [z[a * HALF : (a + 1) * HALF, b * LANES : (b + 1) * LANES] for a, b in pairs(n)], axis=0
    )


def adjoint(block):
    t = block.T
    return jnp.concatenate([t[:HALF], -t[HALF:]], axis=1)


def unpack_to(ref, p):
    n = ref.shape[0] // HALF
    for k, (a, b) in enumerate(pairs(n)):
        block = p[k * HALF : (k + 1) * HALF]
        ref[a * HALF : (a + 1) * HALF, b * LANES : (b + 1) * LANES] = block
        if a != b:
            ref[b * HALF : (b + 1) * HALF, a * LANES : (a + 1) * LANES] = adjoint(block)


def lane_copy(x, lane):
    return jnp.broadcast_to(x[:, lane : lane + 1], (SUB, LANES))


def row_copy(x, row):
    return jnp.broadcast_to(x[row : row + 1, :], (SUB, LANES))


def invert(buf):
    nb = buf.shape[1] // HALF
    groups = HALF // SUB
    lane = lax.broadcasted_iota(jnp.int32, (SUB, LANES), 1)
    sub = lax.broadcasted_iota(jnp.int32, (SUB, LANES), 0)
    low = lane < HALF
    lane_in = jnp.where(low, lane, lane - HALF)

    def at(a, b):
        return (slice(a * HALF, (a + 1) * HALF), slice(b * LANES, (b + 1) * LANES))

    def update(x, t, over, zs, ys):
        cols = (lane_in >= SUB * t) & (lane_in < SUB * (t + 1))
        for g in over:
            lr = [lane_copy(x[g][0], SUB * t + j) for j in range(SUB)]
            li = [lane_copy(x[g][0], HALF + SUB * t + j) for j in range(SUB)]
            new = []
            for b in range(nb):
                base = jnp.where(cols, 0.0, x[g][b]) if b == 0 else x[g][b]
                acc = [lr[j] * zs[j][b] + li[j] * ys[j][b] for j in range(SUB)]
                while len(acc) > 1:
                    acc = [acc[i] + acc[i + 1] for i in range(0, len(acc), 2)]
                new.append(base - acc[0])
            x[g] = new

    def step(i, carry):
        cur, nxt = buf.at[lax.rem(i, 2)], buf.at[lax.rem(i + 1, 2)]
        x = [
            [cur[g * SUB : (g + 1) * SUB, b * LANES : (b + 1) * LANES] for b in range(nb)] for g in range(groups)
        ]
        for t in range(groups):
            z = list(x[t])
            y = [times_i(block) for block in z]
            vr = [lane_copy(z[0], SUB * t + j) for j in range(SUB)]
            vi = [lane_copy(z[0], HALF + SUB * t + j) for j in range(SUB)]
            for p in range(SUB):
                here = sub == p
                col = lane_in == SUB * t + p
                rinv = 1.0 / row_copy(vr[p], p)
                fr = jnp.where(here, 1.0 - rinv, vr[p] * rinv)
                fi = jnp.where(here, 0.0, vi[p] * rinv)
                for j in range(p + 1, SUB):
                    ar, ai = row_copy(vr[j], p), row_copy(vi[j], p)
                    vr[j] = vr[j] - (fr * ar - fi * ai)
                    vi[j] = vi[j] - (fr * ai + fi * ar)
                unit = jnp.where(here, 1.0, 0.0)
                z[0] = jnp.where(col, jnp.where(low, unit, 0.0), z[0])
                y[0] = jnp.where(col, jnp.where(low, 0.0, unit), y[0])
                for b in range(nb):
                    zr, yr = row_copy(z[b], p), row_copy(y[b], p)
                    z[b], y[b] = z[b] - (fr * zr + fi * yr), y[b] - (fr * yr - fi * zr)
            x[t] = z
            zs = [[row_copy(z[b], j) for b in range(nb)] for j in range(SUB)]
            ys = [[row_copy(y[b], j) for b in range(nb)] for j in range(SUB)]
            update(x, t, [(t + 1 + s) % groups for s in range(groups - 1)], zs, ys)
        zp = jnp.concatenate([jnp.concatenate(x[g], axis=1) for g in range(groups)], axis=0)
        for b in range(nb):
            nxt[at(nb - 1, (b - 1) % nb)] = zp[:, b * LANES : (b + 1) * LANES]
        right = jnp.concatenate([zp, times_i(zp)], axis=0)
        change = mm(cur[HALF:, :LANES], right)
        for a in range(1, nb):
            for b in range(nb):
                piece = change[(a - 1) * HALF : a * HALF, b * LANES : (b + 1) * LANES]
                nxt[at(a - 1, (b - 1) % nb)] = -piece if b == 0 else cur[at(a, b)] - piece
        return carry

    lax.fori_loop(0, nb, step, 0)
    return buf.at[nb % 2]


def rows_times(x, z):
    blocks = [x[:, b * LANES : (b + 1) * LANES] for b in range(x.shape[1] // LANES)]
    low = lanes_of(blocks[0]) < HALF
    turned = [pltpu.roll(b, HALF, 1) for b in blocks]
    even = range(0, len(blocks) - 1, 2)
    re = [jnp.where(low, blocks[b], turned[b + 1]) for b in even]
    im = [jnp.where(low, turned[b], blocks[b + 1]) for b in even]
    if len(blocks) % 2:
        re.append(blocks[-1][:, :HALF])
        im.append(turned[-1][:, :HALF])
    both = jnp.concatenate([jnp.concatenate(re, axis=1), jnp.concatenate(im, axis=1)], axis=0)
    got = mm(both, z)
    n = x.shape[0]
    return got[:n] + times_i(got[n:])


def joined(blocks):
    return jnp.concatenate(blocks, axis=0)


def lane_blocks(z):
    return joined([z[:, b * LANES : (b + 1) * LANES] for b in range(z.shape[1] // LANES)])


def from_lane_blocks(ref, start, rows, count):
    return jnp.concatenate([ref[start + b * rows : start + (b + 1) * rows, :] for b in range(count)], axis=1)


def start_kernel(diag_ref, coup_ref, w_ref, t_ref, vv_ref, buf):
    buf[0] = blocked(diag_ref[1])
    w = invert(buf)[...]
    w_ref[...] = w
    second = blocked(coup_ref[1])
    t = mm(second, embed(w))
    t_ref[...] = t
    vv_ref[...] = packed(blocked(diag_ref[0]) - mm_t(t, embed(second)))


def start_side_kernel(coup_ref, next_ref, src_ref, w_ref, t_ref, send_ref, load_ref, wl_ref, back_ref):
    order = w_ref.shape[0]
    first_e = embed(blocked(next_ref[...]))
    t = t_ref[...]
    own = mm(joined([first_rows(first_e.T), blocked(src_ref[1])]), embed(w_ref[...]))
    t2, wl = own[:order], own[order:]
    change = mm(joined([t, t2, wl]), first_e)
    gu = -change[2 * order :]
    gv = blocked(src_ref[0]) - mm_t(wl, embed(blocked(coup_ref[1])))
    load = joined([gu, gv])
    load_ref[...] = load
    send_ref[...] = joined(
        [lane_blocks(-change[:order]), packed(-change[order : 2 * order]), lane_blocks(load)]
    )
    wl_ref[...] = wl
    back_ref[...] = joined([t2, t])


def merge_kernel(theirs_ref, vv_ref, send_ref, w_ref, t_ref, new_vv_ref, buf):
    order = w_ref.shape[0]
    count = w_ref.shape[1] // LANES
    size = vv_ref.shape[0]
    unpack_to(buf.at[0], theirs_ref[...] + send_ref[count * order : count * order + size, :])
    w = invert(buf)[...]
    w_ref[...] = w
    second = from_lane_blocks(send_ref, 0, order, count)
    t = mm(second, embed(w))
    t_ref[...] = t
    new_vv_ref[...] = vv_ref[...] - packed(mm_t(t, embed(second)))


def side_kernel(w_ref, t_ref, mine_ref, theirs_ref, send_ref, load_ref, wl_ref, back_ref):
    order = w_ref.shape[0]
    count = w_ref.shape[1] // LANES
    rest = count * order
    cols = load_ref.shape[0] // 2
    size = send_ref.shape[0] - rest - count * 2 * cols
    first_e = embed(from_lane_blocks(theirs_ref, 0, order, count))
    second_e = embed(from_lane_blocks(mine_ref, 0, order, count))
    my_load = from_lane_blocks(mine_ref, rest + size, 2 * cols, count)
    their_load = from_lane_blocks(theirs_ref, rest + size, 2 * cols, count)
    t = t_ref[...]
    own = mm(joined([first_rows(first_e.T), their_load[cols:] + my_load[:cols]]), embed(w_ref[...]))
    t2, wl = own[:order], own[order:]
    change = mm(joined([t, t2, wl]), first_e)
    gu = their_load[:cols] - change[2 * order :]
    gv = my_load[cols:] - mm_t(wl, second_e)
    load = joined([gu, gv])
    load_ref[...] = load
    send_ref[...] = joined(
        [
            lane_blocks(-change[:order]),
            theirs_ref[rest : rest + size, :] - packed(change[order : 2 * order]),
            lane_blocks(load),
        ]
    )
    wl_ref[...] = wl
    back_ref[...] = joined([t2, t])


def edge_kernel(vv_ref, send_ref, load_ref, uu_ref, h_ref, y_ref, gu_ref, buf):
    order, count = buf.shape[1], buf.shape[2] // LANES
    cols = y_ref.shape[0]
    size = vv_ref.shape[0]
    unpack_to(buf.at[0], vv_ref[...])
    w = invert(buf)[...]
    second_e = embed(from_lane_blocks(send_ref, 0, order, count))
    own = mm(joined([first_rows(second_e.T), load_ref[cols:, :]]), embed(w))
    change = mm(own, second_e)
    uu_ref[...] = send_ref[count * order : count * order + size, :] - packed(change[:order])
    h_ref[...] = own[:order]
    y_ref[...] = own[order:]
    gu_ref[...] = load_ref[:cols, :] - change[order:]


def last_kernel(their_vv_ref, their_load_ref, uu_ref, h_ref, y_ref, gu_ref, out_ref, vl_ref, buf):
    cols = y_ref.shape[0]
    unpack_to(buf.at[0], their_vv_ref[...] + uu_ref[...])
    w = invert(buf)[...]
    mid = rows_times(their_load_ref[cols:, :] + gu_ref[...], w)
    out_ref[...] = joined([jnp.zeros_like(mid), mid])
    vl_ref[...] = y_ref[...] - rows_times(mid, h_ref[...])


def values_of(level, slab_ref, got_ref, prev_ref, vl_ref, wl_ref, back_ref):
    cols = wl_ref.shape[0]
    span = 2 << level
    aimed = lax.rem(slab_ref[0], span) == span // 2
    vu = jnp.where(aimed, got_ref[:cols, :], prev_ref[cols:, :])
    vl = jnp.where(aimed, got_ref[cols:, :], vl_ref[...])
    mid = wl_ref[...] - rows_times(jnp.concatenate([vu, vl], axis=1), back_ref[...])
    return vu, mid, vl


def back_kernel(level, slab_ref, got_ref, prev_ref, vl_ref, wl_ref, back_ref, out_ref, new_vl_ref):
    vu, mid, vl = values_of(level, slab_ref, got_ref, prev_ref, vl_ref, wl_ref, back_ref)
    out_ref[...] = joined([vu, mid])
    new_vl_ref[...] = vl


def end_kernel(slab_ref, got_ref, prev_ref, vl_ref, wl_ref, back_ref, out_ref):
    _, mid, vl = values_of(0, slab_ref, got_ref, prev_ref, vl_ref, wl_ref, back_ref)
    out_ref[0] = unblocked(vl)
    out_ref[1] = unblocked(mid)


def f32(*shape):
    return jax.ShapeDtypeStruct(shape, jnp.float32)


def run(kernel, outs, *args, scalars=0, flops=10**8, scratch=()):
    specs = [pl.BlockSpec(memory_space=pltpu.SMEM)] * scalars
    specs += [pl.BlockSpec(memory_space=pltpu.VMEM)] * (len(args) - scalars)
    return pl.pallas_call(
        kernel,
        out_shape=outs,
        in_specs=specs,
        out_specs=jax.tree.map(lambda _: pl.BlockSpec(memory_space=pltpu.VMEM), outs),
        scratch_shapes=list(scratch),
        compiler_params=pltpu.CompilerParams(vmem_limit_bytes=LIMIT),
        cost_estimate=pl.CostEstimate(flops=flops, bytes_accessed=10**6, transcendentals=0),
    )(*args)


def forward_to(x, axis, distance):
    n = lax.axis_size(axis)
    return lax.ppermute(x, axis, [(i + distance, i) for i in range(0, n, 2 * distance)])


def back_to(x, axis, distance):
    n = lax.axis_size(axis)
    return lax.ppermute(x, axis, [(i, i + distance) for i in range(0, n, 2 * distance)])


def gathered(diag_blocks):
    layer = diag_blocks[0]
    other = diag_blocks[1]
    mine = jnp.where(lax.axis_index("rhs") == 0, layer, other)
    copies = jnp.broadcast_to(mine, (lax.axis_size("orb"), *mine.shape))
    whole = lax.all_to_all(copies, "orb", split_axis=0, concat_axis=0, tiled=True)
    return lax.all_gather(whole.reshape(-1, mine.shape[1]), "rhs")


def local(diag_blocks, couplings, sources):
    order, width = couplings.shape[1:]
    cols = sources.shape[1]
    nb = order // HALF
    size = len(pairs(nb)) * HALF
    whole = f32(order, width)
    vv_shape = f32(size, LANES)
    sides = (
        f32((order + 2 * cols) * width // LANES + size, LANES),
        f32(2 * cols, width),
        f32(cols, width),
        f32(2 * order, width),
    )
    slab = lax.axis_index("slab").astype(jnp.int32).reshape(1)
    heavy, light = 4 * 10**9, 10**9
    n = lax.axis_size("slab")
    following = lax.ppermute(couplings[0], "slab", [(i + 1, i) for i in range(n - 1)])
    buf = [pltpu.VMEM((2, order, width), jnp.float32)]
    pivots = (whole, whole, vv_shape)
    w, t, vv = run(start_kernel, pivots, gathered(diag_blocks), couplings, flops=heavy, scratch=buf)
    levels = n.bit_length() - 1
    stored = []
    for level in range(levels):
        their_vv = forward_to(vv, "slab", 1 << level)
        if level == 0:
            outs = run(start_side_kernel, sides, couplings, following, sources, w, t, flops=light)
        else:
            outs = run(side_kernel, sides, w, t, send, theirs, flops=light)
        send, load, wl, back = outs
        stored.append((wl, back))
        if level < levels - 1:
            theirs = forward_to(send, "slab", 1 << level)
            w, t, vv = run(merge_kernel, pivots, their_vv, vv, send, flops=heavy, scratch=buf)
    theirs = forward_to(load, "slab", 1 << (levels - 1))
    pair = f32(2 * cols, width)
    one = f32(cols, width)
    edge = run(edge_kernel, (vv_shape, whole, one, one), vv, send, load, flops=heavy, scratch=buf)
    values, vl = run(last_kernel, (pair, one), their_vv, theirs, *edge, flops=heavy, scratch=buf)
    for level in reversed(range(levels)):
        got = back_to(values, "slab", 1 << level)
        wl, back = stored[level]
        if level > 0:
            values, vl = run(
                functools.partial(back_kernel, level),
                (pair, one),
                slab, got, values, vl, wl, back,
                scalars=1, flops=10**7,
            )
    return run(end_kernel, f32(2, cols, width), slab, got, values, vl, wl, back, scalars=1, flops=10**7)


def solution(mesh):
    placed = (
        P(("energy", "slab"), "orb", None),
        P(("energy", "slab"), None, None),
        P(("energy", "slab"), ("orb", "rhs"), None),
    )
    return jax.shard_map(
        local,
        mesh=mesh,
        in_specs=placed,
        out_specs=P(("energy", "slab"), ("orb", "rhs"), None),
        check_vma=False,
    )
```

```python
import functools
import jax
import jax.numpy as jnp
from jax import lax
from jax.experimental import pallas as pl
from jax.experimental.pallas import tpu as pltpu
from jax.sharding import PartitionSpec as P


HI = lax.Precision.HIGHEST
LANES = 128
HALF = 64
SUB = 8
LIMIT = 16 * 2**20


def mm(a, b):
    return lax.dot_general(a, b, (((1,), (0,)), ((), ())), precision=HI, preferred_element_type=jnp.float32)


def mm_t(a, b):
    return lax.dot_general(a, b, (((1,), (1,)), ((), ())), precision=HI, preferred_element_type=jnp.float32)


def lanes_of(x):
    return lax.broadcasted_iota(jnp.int32, x.shape, 1)


def times_i(x):
    parts = []
    for b in range(x.shape[1] // LANES):
        blk = x[:, b * LANES : (b + 1) * LANES]
        rolled = pltpu.roll(blk, HALF, 1)
        parts.append(jnp.where(lanes_of(blk) < HALF, -rolled, rolled))
    return jnp.concatenate(parts, axis=1)


def embed(z):
    rows = []
    turned = times_i(z)
    for a in range(z.shape[0] // HALF):
        rows.append(z[a * HALF : (a + 1) * HALF])
        rows.append(turned[a * HALF : (a + 1) * HALF])
    return jnp.concatenate(rows, axis=0)


def first_rows(e):
    return jnp.concatenate([e[a * LANES : a * LANES + HALF] for a in range(e.shape[0] // LANES)], axis=0)


def blocked(x):
    v0, v1, v2 = (x[:, LANES * b : LANES * (b + 1)] for b in range(3))
    low = lanes_of(v0) < HALF
    return jnp.concatenate(
        [jnp.where(low, v0, v1), pltpu.roll(jnp.where(low, v2, v0), HALF, 1), jnp.where(low, v1, v2)], axis=1
    )


def unblocked(x):
    u0, u1, u2 = (x[:, LANES * b : LANES * (b + 1)] for b in range(3))
    low = lanes_of(u0) < HALF
    r1 = pltpu.roll(u1, HALF, 1)
    return jnp.concatenate([jnp.where(low, u0, r1), jnp.where(low, u2, u0), jnp.where(low, r1, u2)], axis=1)


def pairs(n):
    return [(a, b) for a in range(n) for b in range(a, n)]


def packed(z):
    n = z.shape[0] // HALF
    return jnp.concatenate(
        [z[a * HALF : (a + 1) * HALF, b * LANES : (b + 1) * LANES] for a, b in pairs(n)], axis=0
    )


def adjoint(block):
    t = block.T
    return jnp.concatenate([t[:HALF], -t[HALF:]], axis=1)


def unpack_to(ref, p):
    n = ref.shape[0] // HALF
    for k, (a, b) in enumerate(pairs(n)):
        block = p[k * HALF : (k + 1) * HALF]
        ref[a * HALF : (a + 1) * HALF, b * LANES : (b + 1) * LANES] = block
        if a != b:
            ref[b * HALF : (b + 1) * HALF, a * LANES : (a + 1) * LANES] = adjoint(block)


def lane_copy(x, lane):
    return jnp.broadcast_to(x[:, lane : lane + 1], (SUB, LANES))


def row_copy(x, row):
    return jnp.broadcast_to(x[row : row + 1, :], (SUB, LANES))


def invert(buf):
    nb = buf.shape[1] // HALF
    groups = HALF // SUB
    lane = lax.broadcasted_iota(jnp.int32, (SUB, LANES), 1)
    sub = lax.broadcasted_iota(jnp.int32, (SUB, LANES), 0)
    low = lane < HALF
    lane_in = jnp.where(low, lane, lane - HALF)

    def at(a, b):
        return (slice(a * HALF, (a + 1) * HALF), slice(b * LANES, (b + 1) * LANES))

    def update(x, t, over, zs, ys):
        cols = (lane_in >= SUB * t) & (lane_in < SUB * (t + 1))
        for g in over:
            lr = [lane_copy(x[g][0], SUB * t + j) for j in range(SUB)]
            li = [lane_copy(x[g][0], HALF + SUB * t + j) for j in range(SUB)]
            new = []
            for b in range(nb):
                base = jnp.where(cols, 0.0, x[g][b]) if b == 0 else x[g][b]
                acc = [lr[j] * zs[j][b] + li[j] * ys[j][b] for j in range(SUB)]
                while len(acc) > 1:
                    acc = [acc[i] + acc[i + 1] for i in range(0, len(acc), 2)]
                new.append(base - acc[0])
            x[g] = new

    def step(i, carry):
        cur, nxt = buf.at[lax.rem(i, 2)], buf.at[lax.rem(i + 1, 2)]
        x = [
            [cur[g * SUB : (g + 1) * SUB, b * LANES : (b + 1) * LANES] for b in range(nb)] for g in range(groups)
        ]
        for t in range(groups):
            z = list(x[t])
            y = [times_i(block) for block in z]
            vr = [lane_copy(z[0], SUB * t + j) for j in range(SUB)]
            vi = [lane_copy(z[0], HALF + SUB * t + j) for j in range(SUB)]
            for p in range(SUB):
                here = sub == p
                col = lane_in == SUB * t + p
                rinv = 1.0 / row_copy(vr[p], p)
                fr = jnp.where(here, 1.0 - rinv, vr[p] * rinv)
                fi = jnp.where(here, 0.0, vi[p] * rinv)
                for j in range(p + 1, SUB):
                    ar, ai = row_copy(vr[j], p), row_copy(vi[j], p)
                    vr[j] = vr[j] - (fr * ar - fi * ai)
                    vi[j] = vi[j] - (fr * ai + fi * ar)
                unit = jnp.where(here, 1.0, 0.0)
                z[0] = jnp.where(col, jnp.where(low, unit, 0.0), z[0])
                y[0] = jnp.where(col, jnp.where(low, 0.0, unit), y[0])
                for b in range(nb):
                    zr, yr = row_copy(z[b], p), row_copy(y[b], p)
                    z[b], y[b] = z[b] - (fr * zr + fi * yr), y[b] - (fr * yr - fi * zr)
            x[t] = z
            zs = [[row_copy(z[b], j) for b in range(nb)] for j in range(SUB)]
            ys = [[row_copy(y[b], j) for b in range(nb)] for j in range(SUB)]
            update(x, t, [(t + 1 + s) % groups for s in range(groups - 1)], zs, ys)
        zp = jnp.concatenate([jnp.concatenate(x[g], axis=1) for g in range(groups)], axis=0)
        for b in range(nb):
            nxt[at(nb - 1, (b - 1) % nb)] = zp[:, b * LANES : (b + 1) * LANES]
        right = jnp.concatenate([zp, times_i(zp)], axis=0)
        change = mm(cur[HALF:, :LANES], right)
        for a in range(1, nb):
            for b in range(nb):
                piece = change[(a - 1) * HALF : a * HALF, b * LANES : (b + 1) * LANES]
                nxt[at(a - 1, (b - 1) % nb)] = -piece if b == 0 else cur[at(a, b)] - piece
        return carry

    lax.fori_loop(0, nb, step, 0)
    return buf.at[nb % 2]


def rows_times(x, z):
    blocks = [x[:, b * LANES : (b + 1) * LANES] for b in range(x.shape[1] // LANES)]
    low = lanes_of(blocks[0]) < HALF
    turned = [pltpu.roll(b, HALF, 1) for b in blocks]
    even = range(0, len(blocks) - 1, 2)
    re = [jnp.where(low, blocks[b], turned[b + 1]) for b in even]
    im = [jnp.where(low, turned[b], blocks[b + 1]) for b in even]
    if len(blocks) % 2:
        re.append(blocks[-1][:, :HALF])
        im.append(turned[-1][:, :HALF])
    both = jnp.concatenate([jnp.concatenate(re, axis=1), jnp.concatenate(im, axis=1)], axis=0)
    got = mm(both, z)
    n = x.shape[0]
    return got[:n] + times_i(got[n:])


def joined(blocks):
    return jnp.concatenate(blocks, axis=0)


def lane_blocks(z):
    return joined([z[:, b * LANES : (b + 1) * LANES] for b in range(z.shape[1] // LANES)])


def from_lane_blocks(ref, start, rows, count):
    return jnp.concatenate([ref[start + b * rows : start + (b + 1) * rows, :] for b in range(count)], axis=1)


def chained(st, rhs, steps):
    def step(i, carry):
        frm, to, which = steps(i)
        st[to] = mm(st[frm], rhs[which])
        return carry

    return step


def pivot_products(w, second, second_t, st, rhs):
    rhs[0] = embed(w)
    rhs[1] = second_t
    st[0] = second
    lax.fori_loop(0, 2, chained(st, rhs, lambda i: (i, i + 1, i)), 0)
    return st[1], st[2]


def start_kernel(diag_ref, coup_ref, w_ref, t_ref, vv_ref, buf, st, rhs):
    buf[0] = blocked(diag_ref[1])
    w = invert(buf)[...]
    w_ref[...] = w
    second = blocked(coup_ref[1])
    t, change = pivot_products(w, second, embed(second).T, st, rhs)
    t_ref[...] = t
    vv_ref[...] = packed(blocked(diag_ref[0]) - change)


def side_products(w, first_e, loads, t, st, rhs):
    order = w.shape[0]
    rhs[0] = embed(w)
    rhs[1] = first_e
    st[0, :order] = first_rows(first_e.T)
    st[0, order:] = loads
    st[2, :order] = t
    st[2, order:] = jnp.zeros_like(loads)
    lax.fori_loop(0, 3, chained(st, rhs, lambda i: (i, i + 1 + jnp.minimum(i, 1), jnp.minimum(i, 1))), 0)
    return st[1, :order], st[1, order:], st[4, :order], st[3, :order], st[3, order:]


def start_side_kernel(coup_ref, next_ref, src_ref, w_ref, t_ref, send_ref, load_ref, wl_ref, back_ref, st, rhs):
    t = t_ref[...]
    first_e = embed(blocked(next_ref[...]))
    t2, wl, uv, uu, gu = side_products(w_ref[...], first_e, blocked(src_ref[1]), t, st, rhs)
    gv = blocked(src_ref[0]) - mm_t(wl, embed(blocked(coup_ref[1])))
    load = joined([-gu, gv])
    load_ref[...] = load
    send_ref[...] = joined([lane_blocks(-uv), packed(-uu), lane_blocks(load)])
    wl_ref[...] = wl
    back_ref[...] = joined([t2, t])


def on_owner(span, body):
    def kernel(slab_ref, *refs):
        @pl.when(lax.rem(slab_ref[0], span) == 0)
        def _():
            body(*refs)

    return kernel


def merge_kernel(theirs_ref, vv_ref, send_ref, w_ref, t_ref, new_vv_ref, buf, st, rhs):
    order = w_ref.shape[0]
    count = w_ref.shape[1] // LANES
    size = vv_ref.shape[0]
    unpack_to(buf.at[0], theirs_ref[...] + send_ref[count * order : count * order + size, :])
    w = invert(buf)[...]
    w_ref[...] = w
    second = from_lane_blocks(send_ref, 0, order, count)
    t, change = pivot_products(w, second, embed(second).T, st, rhs)
    t_ref[...] = t
    new_vv_ref[...] = vv_ref[...] - packed(change)


def side_kernel(w_ref, t_ref, mine_ref, theirs_ref, send_ref, load_ref, wl_ref, back_ref, st, rhs):
    order = w_ref.shape[0]
    count = w_ref.shape[1] // LANES
    rest = count * order
    cols = load_ref.shape[0] // 2
    size = send_ref.shape[0] - rest - count * 2 * cols
    second_e = embed(from_lane_blocks(mine_ref, 0, order, count))
    my_load = from_lane_blocks(mine_ref, rest + size, 2 * cols, count)
    their_load = from_lane_blocks(theirs_ref, rest + size, 2 * cols, count)
    t = t_ref[...]
    first_e = embed(from_lane_blocks(theirs_ref, 0, order, count))
    t2, wl, uv, uu, gu = side_products(w_ref[...], first_e, their_load[cols:] + my_load[:cols], t, st, rhs)
    gv = my_load[cols:] - mm_t(wl, second_e)
    load = joined([their_load[:cols] - gu, gv])
    load_ref[...] = load
    send_ref[...] = joined([lane_blocks(-uv), theirs_ref[rest : rest + size, :] - packed(uu), lane_blocks(load)])
    wl_ref[...] = wl
    back_ref[...] = joined([t2, t])


def edge_kernel(vv_ref, send_ref, load_ref, uu_ref, h_ref, y_ref, gu_ref, buf, st, rhs):
    order, count = buf.shape[1], buf.shape[2] // LANES
    cols = y_ref.shape[0]
    size = vv_ref.shape[0]
    unpack_to(buf.at[0], vv_ref[...])
    w = invert(buf)[...]
    second_e = embed(from_lane_blocks(send_ref, 0, order, count))
    rhs[0] = embed(w)
    rhs[1] = second_e
    st[0, :order] = first_rows(second_e.T)
    st[0, order:] = load_ref[cols:, :]
    lax.fori_loop(0, 2, chained(st, rhs, lambda i: (i, i + 1, i)), 0)
    uu_ref[...] = send_ref[count * order : count * order + size, :] - packed(st[2, :order])
    h_ref[...] = st[1, :order]
    y_ref[...] = st[1, order:]
    gu_ref[...] = load_ref[:cols, :] - st[2, order:]


def last_kernel(their_vv_ref, their_load_ref, uu_ref, h_ref, y_ref, gu_ref, out_ref, vl_ref, buf):
    cols = y_ref.shape[0]
    unpack_to(buf.at[0], their_vv_ref[...] + uu_ref[...])
    w = invert(buf)[...]
    mid = rows_times(their_load_ref[cols:, :] + gu_ref[...], w)
    out_ref[...] = joined([jnp.zeros_like(mid), mid])
    vl_ref[...] = y_ref[...] - rows_times(mid, h_ref[...])


def values_of(level, slab_ref, got_ref, prev_ref, vl_ref, wl_ref, back_ref):
    cols = wl_ref.shape[0]
    span = 2 << level
    aimed = lax.rem(slab_ref[0], span) == span // 2
    vu = jnp.where(aimed, got_ref[:cols, :], prev_ref[cols:, :])
    vl = jnp.where(aimed, got_ref[cols:, :], vl_ref[...])
    mid = wl_ref[...] - rows_times(jnp.concatenate([vu, vl], axis=1), back_ref[...])
    return vu, mid, vl


def back_kernel(level, slab_ref, got_ref, prev_ref, vl_ref, wl_ref, back_ref, out_ref, new_vl_ref):
    vu, mid, vl = values_of(level, slab_ref, got_ref, prev_ref, vl_ref, wl_ref, back_ref)
    out_ref[...] = joined([vu, mid])
    new_vl_ref[...] = vl


def end_kernel(slab_ref, got_ref, prev_ref, vl_ref, wl_ref, back_ref, out_ref):
    _, mid, vl = values_of(0, slab_ref, got_ref, prev_ref, vl_ref, wl_ref, back_ref)
    out_ref[0] = unblocked(vl)
    out_ref[1] = unblocked(mid)


def f32(*shape):
    return jax.ShapeDtypeStruct(shape, jnp.float32)


def run(kernel, outs, *args, scalars=0, flops=10**8, scratch=()):
    specs = [pl.BlockSpec(memory_space=pltpu.SMEM)] * scalars
    specs += [pl.BlockSpec(memory_space=pltpu.VMEM)] * (len(args) - scalars)
    return pl.pallas_call(
        kernel,
        out_shape=outs,
        in_specs=specs,
        out_specs=jax.tree.map(lambda _: pl.BlockSpec(memory_space=pltpu.VMEM), outs),
        scratch_shapes=list(scratch),
        compiler_params=pltpu.CompilerParams(vmem_limit_bytes=LIMIT),
        cost_estimate=pl.CostEstimate(flops=flops, bytes_accessed=10**6, transcendentals=0),
    )(*args)


def forward_to(x, axis, distance):
    n = lax.axis_size(axis)
    return lax.ppermute(x, axis, [(i + distance, i) for i in range(0, n, 2 * distance)])


def back_to(x, axis, distance):
    n = lax.axis_size(axis)
    return lax.ppermute(x, axis, [(i, i + distance) for i in range(0, n, 2 * distance)])


def gathered(diag_blocks):
    layer = diag_blocks[0]
    other = diag_blocks[1]
    mine = jnp.where(lax.axis_index("rhs") == 0, layer, other)
    copies = jnp.broadcast_to(mine, (lax.axis_size("orb"), *mine.shape))
    whole = lax.all_to_all(copies, "orb", split_axis=0, concat_axis=0, tiled=True)
    return lax.all_gather(whole.reshape(-1, mine.shape[1]), "rhs")


def local(diag_blocks, couplings, sources):
    order, width = couplings.shape[1:]
    cols = sources.shape[1]
    nb = order // HALF
    size = len(pairs(nb)) * HALF
    whole = f32(order, width)
    vv_shape = f32(size, LANES)
    sides = (
        f32((order + 2 * cols) * width // LANES + size, LANES),
        f32(2 * cols, width),
        f32(cols, width),
        f32(2 * order, width),
    )
    slab = lax.axis_index("slab").astype(jnp.int32).reshape(1)
    heavy, light = 4 * 10**9, 10**9
    n = lax.axis_size("slab")
    following = lax.ppermute(couplings[0], "slab", [(i + 1, i) for i in range(n - 1)])
    levels = n.bit_length() - 1
    rhs = pltpu.VMEM((2, width, width), jnp.float32)
    buf = pltpu.VMEM((2, order, width), jnp.float32)
    for_pivot = (buf, pltpu.VMEM((3, order, width), jnp.float32), rhs)
    for_side = (pltpu.VMEM((5, order + cols, width), jnp.float32), rhs)
    for_edge = (buf, pltpu.VMEM((3, order + cols, width), jnp.float32), rhs)
    pivots = (whole, whole, vv_shape)
    pair = f32(2 * cols, width)
    one = f32(cols, width)

    def on(level, kernel, outs, *args, flops, scratch):
        return run(on_owner(1 << level, kernel), outs, slab, *args, scalars=1, flops=flops, scratch=scratch)

    w, t, vv = run(start_kernel, pivots, gathered(diag_blocks), couplings, flops=heavy, scratch=for_pivot)
    stored = []
    for level in range(levels):
        their_vv = forward_to(vv, "slab", 1 << level)
        if level == 0:
            outs = run(
                start_side_kernel, sides, couplings, following, sources, w, t, flops=light, scratch=for_side
            )
        else:
            outs = on(level, side_kernel, sides, w, t, send, theirs, flops=light, scratch=for_side)
        send, load, wl, back = outs
        stored.append((wl, back))
        if level < levels - 1:
            theirs = forward_to(send, "slab", 1 << level)
            w, t, vv = on(
                level + 1, merge_kernel, pivots, their_vv, vv, send, flops=heavy, scratch=for_pivot
            )
    theirs = forward_to(load, "slab", 1 << (levels - 1))
    edge = on(
        levels, edge_kernel, (vv_shape, whole, one, one), vv, send, load, flops=heavy, scratch=for_edge
    )
    values, vl = on(
        levels, last_kernel, (pair, one), their_vv, theirs, *edge, flops=heavy, scratch=(buf,)
    )
    for level in reversed(range(levels)):
        got = back_to(values, "slab", 1 << level)
        wl, back = stored[level]
        if level > 0:
            values, vl = run(
                functools.partial(back_kernel, level),
                (pair, one),
                slab, got, values, vl, wl, back,
                scalars=1, flops=10**7,
            )
    return run(end_kernel, f32(2, cols, width), slab, got, values, vl, wl, back, scalars=1, flops=10**7)


def solution(mesh):
    placed = (
        P(("energy", "slab"), "orb", None),
        P(("energy", "slab"), None, None),
        P(("energy", "slab"), ("orb", "rhs"), None),
    )
    return jax.shard_map(
        local,
        mesh=mesh,
        in_specs=placed,
        out_specs=P(("energy", "slab"), ("orb", "rhs"), None),
        check_vma=False,
    )
```

```python
import functools
import jax
import jax.numpy as jnp
from jax import lax
from jax.experimental import pallas as pl
from jax.experimental.pallas import tpu as pltpu
from jax.sharding import PartitionSpec as P


HI = lax.Precision.HIGHEST
LANES = 128
HALF = 64
SUB = 8
LIMIT = 16 * 2**20


def mm(a, b):
    return lax.dot_general(a, b, (((1,), (0,)), ((), ())), precision=HI, preferred_element_type=jnp.float32)


def mm_t(a, b):
    return lax.dot_general(a, b, (((1,), (1,)), ((), ())), precision=HI, preferred_element_type=jnp.float32)


def lanes_of(x):
    return lax.broadcasted_iota(jnp.int32, x.shape, 1)


def times_i(x):
    parts = []
    for b in range(x.shape[1] // LANES):
        blk = x[:, b * LANES : (b + 1) * LANES]
        rolled = pltpu.roll(blk, HALF, 1)
        parts.append(jnp.where(lanes_of(blk) < HALF, -rolled, rolled))
    return jnp.concatenate(parts, axis=1)


def embed(z):
    rows = []
    turned = times_i(z)
    for a in range(z.shape[0] // HALF):
        rows.append(z[a * HALF : (a + 1) * HALF])
        rows.append(turned[a * HALF : (a + 1) * HALF])
    return jnp.concatenate(rows, axis=0)


def first_rows(e):
    return jnp.concatenate([e[a * LANES : a * LANES + HALF] for a in range(e.shape[0] // LANES)], axis=0)


def blocked(x):
    v0, v1, v2 = (x[:, LANES * b : LANES * (b + 1)] for b in range(3))
    low = lanes_of(v0) < HALF
    return jnp.concatenate(
        [jnp.where(low, v0, v1), pltpu.roll(jnp.where(low, v2, v0), HALF, 1), jnp.where(low, v1, v2)], axis=1
    )


def unblocked(x):
    u0, u1, u2 = (x[:, LANES * b : LANES * (b + 1)] for b in range(3))
    low = lanes_of(u0) < HALF
    r1 = pltpu.roll(u1, HALF, 1)
    return jnp.concatenate([jnp.where(low, u0, r1), jnp.where(low, u2, u0), jnp.where(low, r1, u2)], axis=1)


def pairs(n):
    return [(a, b) for a in range(n) for b in range(a, n)]


def packed(z):
    n = z.shape[0] // HALF
    return jnp.concatenate(
        [z[a * HALF : (a + 1) * HALF, b * LANES : (b + 1) * LANES] for a, b in pairs(n)], axis=0
    )


def adjoint(block):
    t = block.T
    return jnp.concatenate([t[:HALF], -t[HALF:]], axis=1)


def unpack_to(ref, p):
    n = ref.shape[0] // HALF
    for k, (a, b) in enumerate(pairs(n)):
        block = p[k * HALF : (k + 1) * HALF]
        ref[a * HALF : (a + 1) * HALF, b * LANES : (b + 1) * LANES] = block
        if a != b:
            ref[b * HALF : (b + 1) * HALF, a * LANES : (a + 1) * LANES] = adjoint(block)


def lane_copy(x, lane):
    return jnp.broadcast_to(x[:, lane : lane + 1], (SUB, LANES))


def row_copy(x, row):
    return jnp.broadcast_to(x[row : row + 1, :], (SUB, LANES))


def invert(buf):
    nb = buf.shape[1] // HALF
    groups = HALF // SUB
    lane = lax.broadcasted_iota(jnp.int32, (SUB, LANES), 1)
    sub = lax.broadcasted_iota(jnp.int32, (SUB, LANES), 0)
    low = lane < HALF
    lane_in = jnp.where(low, lane, lane - HALF)

    def at(a, b):
        return (slice(a * HALF, (a + 1) * HALF), slice(b * LANES, (b + 1) * LANES))

    def step(i, carry):
        cur, nxt = buf.at[lax.rem(i, 2)], buf.at[lax.rem(i + 1, 2)]
        x = [cur[g * SUB : (g + 1) * SUB, :LANES] for g in range(groups)]
        for t in range(groups):
            z = x[t]
            y = times_i(z)
            vr = [lane_copy(z, SUB * t + j) for j in range(SUB)]
            vi = [lane_copy(z, HALF + SUB * t + j) for j in range(SUB)]
            for p in range(SUB):
                here = sub == p
                col = lane_in == SUB * t + p
                rinv = 1.0 / row_copy(vr[p], p)
                fr = jnp.where(here, 1.0 - rinv, vr[p] * rinv)
                fi = jnp.where(here, 0.0, vi[p] * rinv)
                for j in range(p + 1, SUB):
                    ar, ai = row_copy(vr[j], p), row_copy(vi[j], p)
                    vr[j] = vr[j] - (fr * ar - fi * ai)
                    vi[j] = vi[j] - (fr * ai + fi * ar)
                unit = jnp.where(here, 1.0, 0.0)
                z = jnp.where(col, jnp.where(low, unit, 0.0), z)
                y = jnp.where(col, jnp.where(low, 0.0, unit), y)
                zr, yr = row_copy(z, p), row_copy(y, p)
                z, y = z - (fr * zr + fi * yr), y - (fr * yr - fi * zr)
            x[t] = z
            zs = [row_copy(z, j) for j in range(SUB)]
            ys = [row_copy(y, j) for j in range(SUB)]
            cols = (lane_in >= SUB * t) & (lane_in < SUB * (t + 1))
            for g in [(t + 1 + s) % groups for s in range(groups - 1)]:
                acc = [
                    lane_copy(x[g], SUB * t + j) * zs[j] + lane_copy(x[g], HALF + SUB * t + j) * ys[j]
                    for j in range(SUB)
                ]
                while len(acc) > 1:
                    acc = [acc[q] + acc[q + 1] for q in range(0, len(acc), 2)]
                x[g] = jnp.where(cols, 0.0, x[g]) - acc[0]
        d = jnp.concatenate(x, axis=0)
        rest = cur[:HALF, LANES:]
        rest = mm(d, jnp.concatenate([rest, times_i(rest)], axis=0))
        zp = jnp.concatenate([d, rest], axis=1)
        for b in range(nb):
            nxt[at(nb - 1, (b - 1) % nb)] = zp[:, b * LANES : (b + 1) * LANES]
        change = mm(cur[HALF:, :LANES], jnp.concatenate([zp, times_i(zp)], axis=0))
        for a in range(1, nb):
            for b in range(nb):
                piece = change[(a - 1) * HALF : a * HALF, b * LANES : (b + 1) * LANES]
                nxt[at(a - 1, (b - 1) % nb)] = -piece if b == 0 else cur[at(a, b)] - piece
        return carry

    lax.fori_loop(0, nb, step, 0)
    return buf.at[nb % 2]


def rows_times(x, z):
    blocks = [x[:, b * LANES : (b + 1) * LANES] for b in range(x.shape[1] // LANES)]
    low = lanes_of(blocks[0]) < HALF
    turned = [pltpu.roll(b, HALF, 1) for b in blocks]
    even = range(0, len(blocks) - 1, 2)
    re = [jnp.where(low, blocks[b], turned[b + 1]) for b in even]
    im = [jnp.where(low, turned[b], blocks[b + 1]) for b in even]
    if len(blocks) % 2:
        re.append(blocks[-1][:, :HALF])
        im.append(turned[-1][:, :HALF])
    both = jnp.concatenate([jnp.concatenate(re, axis=1), jnp.concatenate(im, axis=1)], axis=0)
    got = mm(both, z)
    n = x.shape[0]
    return got[:n] + times_i(got[n:])


def joined(blocks):
    return jnp.concatenate(blocks, axis=0)


def lane_blocks(z):
    return joined([z[:, b * LANES : (b + 1) * LANES] for b in range(z.shape[1] // LANES)])


def from_lane_blocks(ref, start, rows, count):
    return jnp.concatenate([ref[start + b * rows : start + (b + 1) * rows, :] for b in range(count)], axis=1)


def chained(st, rhs, steps):
    def step(i, carry):
        frm, to, which = steps(i)
        st[to] = mm(st[frm], rhs[which])
        return carry

    return step


def start_kernel(diag_ref, coup_ref, w_ref, t_ref, vv_ref, buf):
    buf[0] = blocked(diag_ref[1])
    w = invert(buf)[...]
    w_ref[...] = w
    second = blocked(coup_ref[1])
    t = mm(second, embed(w))
    t_ref[...] = t
    vv_ref[...] = packed(blocked(diag_ref[0]) - mm_t(t, embed(second)))


def side_products(w, first_e, loads, t, st, rhs):
    order = w.shape[0]
    rhs[0] = embed(w)
    rhs[1] = first_e
    st[0, :order] = first_rows(first_e.T)
    st[0, order:] = loads
    st[2, :order] = t
    st[2, order:] = jnp.zeros_like(loads)
    lax.fori_loop(0, 3, chained(st, rhs, lambda i: (i, i + 1 + jnp.minimum(i, 1), jnp.minimum(i, 1))), 0)
    return st[1, :order], st[1, order:], st[4, :order], st[3, :order], st[3, order:]


def start_side_kernel(coup_ref, next_ref, src_ref, w_ref, t_ref, send_ref, load_ref, wl_ref, back_ref, st, rhs):
    t = t_ref[...]
    first_e = embed(blocked(next_ref[...]))
    t2, wl, uv, uu, gu = side_products(w_ref[...], first_e, blocked(src_ref[1]), t, st, rhs)
    gv = blocked(src_ref[0]) - mm_t(wl, embed(blocked(coup_ref[1])))
    load = joined([-gu, gv])
    load_ref[...] = load
    send_ref[...] = joined([lane_blocks(-uv), packed(-uu), lane_blocks(load)])
    wl_ref[...] = wl
    back_ref[...] = joined([t2, t])


def on_owner(span, body):
    def kernel(slab_ref, *refs):
        @pl.when(lax.rem(slab_ref[0], span) == 0)
        def _():
            body(*refs)

    return kernel


def merge_kernel(theirs_ref, vv_ref, send_ref, w_ref, t_ref, new_vv_ref, buf):
    order = w_ref.shape[0]
    count = w_ref.shape[1] // LANES
    size = vv_ref.shape[0]
    unpack_to(buf.at[0], theirs_ref[...] + send_ref[count * order : count * order + size, :])
    w = invert(buf)[...]
    w_ref[...] = w
    second = from_lane_blocks(send_ref, 0, order, count)
    t = mm(second, embed(w))
    t_ref[...] = t
    new_vv_ref[...] = vv_ref[...] - packed(mm_t(t, embed(second)))


def side_kernel(w_ref, t_ref, mine_ref, theirs_ref, send_ref, load_ref, wl_ref, back_ref, st, rhs):
    order = w_ref.shape[0]
    count = w_ref.shape[1] // LANES
    rest = count * order
    cols = load_ref.shape[0] // 2
    size = send_ref.shape[0] - rest - count * 2 * cols
    second_e = embed(from_lane_blocks(mine_ref, 0, order, count))
    my_load = from_lane_blocks(mine_ref, rest + size, 2 * cols, count)
    their_load = from_lane_blocks(theirs_ref, rest + size, 2 * cols, count)
    t = t_ref[...]
    first_e = embed(from_lane_blocks(theirs_ref, 0, order, count))
    t2, wl, uv, uu, gu = side_products(w_ref[...], first_e, their_load[cols:] + my_load[:cols], t, st, rhs)
    gv = my_load[cols:] - mm_t(wl, second_e)
    load = joined([their_load[:cols] - gu, gv])
    load_ref[...] = load
    send_ref[...] = joined([lane_blocks(-uv), theirs_ref[rest : rest + size, :] - packed(uu), lane_blocks(load)])
    wl_ref[...] = wl
    back_ref[...] = joined([t2, t])


def edge_kernel(vv_ref, send_ref, load_ref, uu_ref, h_ref, y_ref, gu_ref, buf):
    order, count = buf.shape[1], buf.shape[2] // LANES
    cols = y_ref.shape[0]
    size = vv_ref.shape[0]
    unpack_to(buf.at[0], vv_ref[...])
    w = invert(buf)[...]
    second_e = embed(from_lane_blocks(send_ref, 0, order, count))
    own = mm(joined([first_rows(second_e.T), load_ref[cols:, :]]), embed(w))
    change = mm(own, second_e)
    uu_ref[...] = send_ref[count * order : count * order + size, :] - packed(change[:order])
    h_ref[...] = own[:order]
    y_ref[...] = own[order:]
    gu_ref[...] = load_ref[:cols, :] - change[order:]


def last_kernel(their_vv_ref, their_load_ref, uu_ref, h_ref, y_ref, gu_ref, out_ref, vl_ref, buf):
    cols = y_ref.shape[0]
    unpack_to(buf.at[0], their_vv_ref[...] + uu_ref[...])
    w = invert(buf)[...]
    mid = rows_times(their_load_ref[cols:, :] + gu_ref[...], w)
    out_ref[...] = joined([jnp.zeros_like(mid), mid])
    vl_ref[...] = y_ref[...] - rows_times(mid, h_ref[...])


def values_of(level, slab_ref, got_ref, prev_ref, vl_ref, wl_ref, back_ref):
    cols = wl_ref.shape[0]
    span = 2 << level
    aimed = lax.rem(slab_ref[0], span) == span // 2
    vu = jnp.where(aimed, got_ref[:cols, :], prev_ref[cols:, :])
    vl = jnp.where(aimed, got_ref[cols:, :], vl_ref[...])
    mid = wl_ref[...] - rows_times(jnp.concatenate([vu, vl], axis=1), back_ref[...])
    return vu, mid, vl


def back_kernel(level, slab_ref, got_ref, prev_ref, vl_ref, wl_ref, back_ref, out_ref, new_vl_ref):
    vu, mid, vl = values_of(level, slab_ref, got_ref, prev_ref, vl_ref, wl_ref, back_ref)
    out_ref[...] = joined([vu, mid])
    new_vl_ref[...] = vl


def end_kernel(slab_ref, got_ref, prev_ref, vl_ref, wl_ref, back_ref, out_ref):
    _, mid, vl = values_of(0, slab_ref, got_ref, prev_ref, vl_ref, wl_ref, back_ref)
    out_ref[0] = unblocked(vl)
    out_ref[1] = unblocked(mid)


def f32(*shape):
    return jax.ShapeDtypeStruct(shape, jnp.float32)


def run(kernel, outs, *args, scalars=0, flops=10**8, scratch=()):
    specs = [pl.BlockSpec(memory_space=pltpu.SMEM)] * scalars
    specs += [pl.BlockSpec(memory_space=pltpu.VMEM)] * (len(args) - scalars)
    return pl.pallas_call(
        kernel,
        out_shape=outs,
        in_specs=specs,
        out_specs=jax.tree.map(lambda _: pl.BlockSpec(memory_space=pltpu.VMEM), outs),
        scratch_shapes=list(scratch),
        compiler_params=pltpu.CompilerParams(vmem_limit_bytes=LIMIT),
        cost_estimate=pl.CostEstimate(flops=flops, bytes_accessed=10**6, transcendentals=0),
    )(*args)


def forward_to(x, axis, distance):
    n = lax.axis_size(axis)
    return lax.ppermute(x, axis, [(i + distance, i) for i in range(0, n, 2 * distance)])


def back_to(x, axis, distance):
    n = lax.axis_size(axis)
    return lax.ppermute(x, axis, [(i, i + distance) for i in range(0, n, 2 * distance)])


def gathered(diag_blocks):
    width = diag_blocks.shape[2]
    copies = [jnp.broadcast_to(layer, (lax.axis_size("orb"), *layer.shape)) for layer in diag_blocks]
    copies = jnp.where(lax.axis_index("rhs") == 0, copies[0], copies[1])
    whole = lax.all_to_all(copies, "orb", split_axis=0, concat_axis=0, tiled=True)
    return lax.all_gather(whole.reshape(-1, width), "rhs")


def local(diag_blocks, couplings, sources):
    order, width = couplings.shape[1:]
    cols = sources.shape[1]
    nb = order // HALF
    size = len(pairs(nb)) * HALF
    whole = f32(order, width)
    vv_shape = f32(size, LANES)
    sides = (
        f32((order + 2 * cols) * width // LANES + size, LANES),
        f32(2 * cols, width),
        f32(cols, width),
        f32(2 * order, width),
    )
    slab = lax.axis_index("slab").astype(jnp.int32).reshape(1)
    heavy, light = 4 * 10**9, 10**9
    n = lax.axis_size("slab")
    following = lax.ppermute(couplings[0], "slab", [(i + 1, i) for i in range(n - 1)])
    levels = n.bit_length() - 1
    rhs = pltpu.VMEM((2, width, width), jnp.float32)
    buf = pltpu.VMEM((2, order, width), jnp.float32)
    for_pivot = (buf,)
    for_side = (pltpu.VMEM((5, order + cols, width), jnp.float32), rhs)
    pivots = (whole, whole, vv_shape)
    pair = f32(2 * cols, width)
    one = f32(cols, width)

    def on(level, kernel, outs, *args, flops, scratch):
        return run(on_owner(1 << level, kernel), outs, slab, *args, scalars=1, flops=flops, scratch=scratch)

    w, t, vv = run(start_kernel, pivots, gathered(diag_blocks), couplings, flops=heavy, scratch=for_pivot)
    stored = []
    for level in range(levels):
        their_vv = forward_to(vv, "slab", 1 << level)
        if level == 0:
            outs = run(
                start_side_kernel, sides, couplings, following, sources, w, t, flops=light, scratch=for_side
            )
        else:
            outs = on(level, side_kernel, sides, w, t, send, theirs, flops=light, scratch=for_side)
        send, load, wl, back = outs
        stored.append((wl, back))
        if level < levels - 1:
            theirs = forward_to(send, "slab", 1 << level)
            w, t, vv = on(
                level + 1, merge_kernel, pivots, their_vv, vv, send, flops=heavy, scratch=for_pivot
            )
    theirs = forward_to(load, "slab", 1 << (levels - 1))
    edge = on(
        levels, edge_kernel, (vv_shape, whole, one, one), vv, send, load, flops=heavy, scratch=for_pivot
    )
    values, vl = on(
        levels, last_kernel, (pair, one), their_vv, theirs, *edge, flops=heavy, scratch=for_pivot
    )
    for level in reversed(range(levels)):
        got = back_to(values, "slab", 1 << level)
        wl, back = stored[level]
        if level > 0:
            values, vl = run(
                functools.partial(back_kernel, level),
                (pair, one),
                slab, got, values, vl, wl, back,
                scalars=1, flops=10**7,
            )
    return run(end_kernel, f32(2, cols, width), slab, got, values, vl, wl, back, scalars=1, flops=10**7)


def solution(mesh):
    placed = (
        P(("energy", "slab"), "orb", None),
        P(("energy", "slab"), None, None),
        P(("energy", "slab"), ("orb", "rhs"), None),
    )
    return jax.shard_map(
        local,
        mesh=mesh,
        in_specs=placed,
        out_specs=P(("energy", "slab"), ("orb", "rhs"), None),
        check_vma=False,
    )
```

```python
import functools
import jax
import jax.numpy as jnp
from jax import lax
from jax.experimental import pallas as pl
from jax.experimental.pallas import tpu as pltpu
from jax.sharding import PartitionSpec as P


HI = lax.Precision.HIGHEST
LANES = 128
HALF = 64
SUB = 8
LIMIT = 16 * 2**20


def mm(a, b):
    return lax.dot_general(a, b, (((1,), (0,)), ((), ())), precision=HI, preferred_element_type=jnp.float32)


def mm_t(a, b):
    return lax.dot_general(a, b, (((1,), (1,)), ((), ())), precision=HI, preferred_element_type=jnp.float32)


def lanes_of(x):
    return lax.broadcasted_iota(jnp.int32, x.shape, 1)


def times_i(x):
    parts = []
    for b in range(x.shape[1] // LANES):
        blk = x[:, b * LANES : (b + 1) * LANES]
        rolled = pltpu.roll(blk, HALF, 1)
        parts.append(jnp.where(lanes_of(blk) < HALF, -rolled, rolled))
    return jnp.concatenate(parts, axis=1)


def embed(z):
    rows = []
    turned = times_i(z)
    for a in range(z.shape[0] // HALF):
        rows.append(z[a * HALF : (a + 1) * HALF])
        rows.append(turned[a * HALF : (a + 1) * HALF])
    return jnp.concatenate(rows, axis=0)


def first_rows(e):
    return jnp.concatenate([e[a * LANES : a * LANES + HALF] for a in range(e.shape[0] // LANES)], axis=0)


def blocked(x):
    v0, v1, v2 = (x[:, LANES * b : LANES * (b + 1)] for b in range(3))
    low = lanes_of(v0) < HALF
    return jnp.concatenate(
        [jnp.where(low, v0, v1), pltpu.roll(jnp.where(low, v2, v0), HALF, 1), jnp.where(low, v1, v2)], axis=1
    )


def unblocked(x):
    u0, u1, u2 = (x[:, LANES * b : LANES * (b + 1)] for b in range(3))
    low = lanes_of(u0) < HALF
    r1 = pltpu.roll(u1, HALF, 1)
    return jnp.concatenate([jnp.where(low, u0, r1), jnp.where(low, u2, u0), jnp.where(low, r1, u2)], axis=1)


def pairs(n):
    return [(a, b) for a in range(n) for b in range(a + 1, n)]


def packed_rows(n):
    return len(pairs(n)) * HALF + n // 2 * HALF + n % 2 * (HALF // 2)


def halves_of(block):
    low = lanes_of(block) < HALF
    row = lax.broadcasted_iota(jnp.int32, block.shape, 0)
    col = jnp.where(low, lanes_of(block), lanes_of(block) - HALF)
    return low, row, col


def hermitian_low(block):
    _, row, col = halves_of(block)
    return jnp.where(row <= col, block, pltpu.roll(block, HALF, 1))


def hermitian_high(block):
    _, row, col = halves_of(block)
    return jnp.where(row <= col, pltpu.roll(block, HALF, 1), block)


def packed(z):
    n = z.shape[0] // HALF

    def block(a, b):
        return z[a * HALF : (a + 1) * HALF, b * LANES : (b + 1) * LANES]

    parts = [block(a, b) for a, b in pairs(n)]
    for a in range(0, n - 1, 2):
        first, second = hermitian_low(block(a, a)), hermitian_high(block(a + 1, a + 1))
        parts.append(jnp.where(lanes_of(first) < HALF, first, second))
    if n % 2:
        last = hermitian_low(block(n - 1, n - 1))
        top, bottom = last[: HALF // 2], pltpu.roll(last[HALF // 2 :], HALF, 1)
        parts.append(jnp.where(lanes_of(top) < HALF, top, bottom))
    return jnp.concatenate(parts, axis=0)


def hermitian(half):
    low, row, col = halves_of(half)
    twice = jnp.where(low, half, pltpu.roll(half, HALF, 1))
    t = twice.T
    flipped = jnp.concatenate([t[:HALF], t[HALF:]], axis=1)
    re = jnp.where(row <= col, twice, flipped)
    im = jnp.where(row > col, twice, jnp.where(row < col, -flipped, 0.0))
    return jnp.where(low, re, im)


def adjoint(block):
    t = block.T
    return jnp.concatenate([t[:HALF], -t[HALF:]], axis=1)


def unpack_to(ref, p):
    n = ref.shape[0] // HALF

    def put(a, b, block):
        ref[a * HALF : (a + 1) * HALF, b * LANES : (b + 1) * LANES] = block

    for k, (a, b) in enumerate(pairs(n)):
        block = p[k * HALF : (k + 1) * HALF]
        put(a, b, block)
        put(b, a, adjoint(block))
    start = len(pairs(n)) * HALF
    for a in range(0, n - 1, 2):
        block = p[start : start + HALF]
        put(a, a, hermitian(block))
        put(a + 1, a + 1, hermitian(pltpu.roll(block, HALF, 1)))
        start += HALF
    if n % 2:
        block = p[start : start + HALF // 2]
        put(n - 1, n - 1, hermitian(jnp.concatenate([block, pltpu.roll(block, HALF, 1)], axis=0)))


def lane_copy(x, lane):
    return jnp.broadcast_to(x[:, lane : lane + 1], (SUB, LANES))


def row_copy(x, row):
    return jnp.broadcast_to(x[row : row + 1, :], (SUB, LANES))


def invert(buf):
    nb = buf.shape[1] // HALF
    groups = HALF // SUB
    lane = lax.broadcasted_iota(jnp.int32, (SUB, LANES), 1)
    sub = lax.broadcasted_iota(jnp.int32, (SUB, LANES), 0)
    low = lane < HALF
    lane_in = jnp.where(low, lane, lane - HALF)

    def at(a, b):
        return (slice(a * HALF, (a + 1) * HALF), slice(b * LANES, (b + 1) * LANES))

    def step(i, carry):
        cur, nxt = buf.at[lax.rem(i, 2)], buf.at[lax.rem(i + 1, 2)]
        x = [cur[g * SUB : (g + 1) * SUB, :LANES] for g in range(groups)]
        for t in range(groups):
            z = x[t]
            y = times_i(z)
            vr = [lane_copy(z, SUB * t + j) for j in range(SUB)]
            vi = [lane_copy(z, HALF + SUB * t + j) for j in range(SUB)]
            for p in range(SUB):
                here = sub == p
                col = lane_in == SUB * t + p
                rinv = 1.0 / row_copy(vr[p], p)
                fr = jnp.where(here, 1.0 - rinv, vr[p] * rinv)
                fi = jnp.where(here, 0.0, vi[p] * rinv)
                for j in range(p + 1, SUB):
                    ar, ai = row_copy(vr[j], p), row_copy(vi[j], p)
                    vr[j] = vr[j] - (fr * ar - fi * ai)
                    vi[j] = vi[j] - (fr * ai + fi * ar)
                unit = jnp.where(here, 1.0, 0.0)
                z = jnp.where(col, jnp.where(low, unit, 0.0), z)
                y = jnp.where(col, jnp.where(low, 0.0, unit), y)
                zr, yr = row_copy(z, p), row_copy(y, p)
                z, y = z - (fr * zr + fi * yr), y - (fr * yr - fi * zr)
            x[t] = z
            zs = [row_copy(z, j) for j in range(SUB)]
            ys = [row_copy(y, j) for j in range(SUB)]
            cols = (lane_in >= SUB * t) & (lane_in < SUB * (t + 1))
            for g in [(t + 1 + s) % groups for s in range(groups - 1)]:
                acc = [
                    lane_copy(x[g], SUB * t + j) * zs[j] + lane_copy(x[g], HALF + SUB * t + j) * ys[j]
                    for j in range(SUB)
                ]
                while len(acc) > 1:
                    acc = [acc[q] + acc[q + 1] for q in range(0, len(acc), 2)]
                x[g] = jnp.where(cols, 0.0, x[g]) - acc[0]
        d = jnp.concatenate(x, axis=0)
        rest = cur[:HALF, LANES:]
        rest = mm(d, jnp.concatenate([rest, times_i(rest)], axis=0))
        zp = jnp.concatenate([d, rest], axis=1)
        for b in range(nb):
            nxt[at(nb - 1, (b - 1) % nb)] = zp[:, b * LANES : (b + 1) * LANES]
        change = mm(cur[HALF:, :LANES], jnp.concatenate([zp, times_i(zp)], axis=0))
        for a in range(1, nb):
            for b in range(nb):
                piece = change[(a - 1) * HALF : a * HALF, b * LANES : (b + 1) * LANES]
                nxt[at(a - 1, (b - 1) % nb)] = -piece if b == 0 else cur[at(a, b)] - piece
        return carry

    lax.fori_loop(0, nb, step, 0)
    return buf.at[nb % 2]


def rows_times(x, z):
    blocks = [x[:, b * LANES : (b + 1) * LANES] for b in range(x.shape[1] // LANES)]
    low = lanes_of(blocks[0]) < HALF
    turned = [pltpu.roll(b, HALF, 1) for b in blocks]
    even = range(0, len(blocks) - 1, 2)
    re = [jnp.where(low, blocks[b], turned[b + 1]) for b in even]
    im = [jnp.where(low, turned[b], blocks[b + 1]) for b in even]
    if len(blocks) % 2:
        re.append(blocks[-1][:, :HALF])
        im.append(turned[-1][:, :HALF])
    both = jnp.concatenate([jnp.concatenate(re, axis=1), jnp.concatenate(im, axis=1)], axis=0)
    got = mm(both, z)
    n = x.shape[0]
    return got[:n] + times_i(got[n:])


def joined(blocks):
    return jnp.concatenate(blocks, axis=0)


def lane_blocks(z):
    return joined([z[:, b * LANES : (b + 1) * LANES] for b in range(z.shape[1] // LANES)])


def from_lane_blocks(ref, start, rows, count):
    return jnp.concatenate([ref[start + b * rows : start + (b + 1) * rows, :] for b in range(count)], axis=1)


def chained(st, rhs, steps):
    def step(i, carry):
        frm, to, which = steps(i)
        st[to] = mm(st[frm], rhs[which])
        return carry

    return step


def start_kernel(diag_ref, coup_ref, w_ref, t_ref, vv_ref, buf):
    buf[0] = blocked(diag_ref[1])
    w = invert(buf)[...]
    w_ref[...] = w
    second = blocked(coup_ref[1])
    t = mm(second, embed(w))
    t_ref[...] = t
    vv_ref[...] = packed(blocked(diag_ref[0]) - mm_t(t, embed(second)))


def side_products(w, first_e, loads, t, st, rhs):
    order = w.shape[0]
    rhs[0] = embed(w)
    rhs[1] = first_e
    st[0, :order] = first_rows(first_e.T)
    st[0, order:] = loads
    st[2, :order] = t
    st[2, order:] = jnp.zeros_like(loads)
    lax.fori_loop(0, 3, chained(st, rhs, lambda i: (i, i + 1 + jnp.minimum(i, 1), jnp.minimum(i, 1))), 0)
    return st[1, :order], st[1, order:], st[4, :order], st[3, :order], st[3, order:]


def start_side_kernel(coup_ref, next_ref, src_ref, w_ref, t_ref, send_ref, load_ref, wl_ref, back_ref, st, rhs):
    t = t_ref[...]
    first_e = embed(blocked(next_ref[...]))
    t2, wl, uv, uu, gu = side_products(w_ref[...], first_e, blocked(src_ref[1]), t, st, rhs)
    gv = blocked(src_ref[0]) - mm_t(wl, embed(blocked(coup_ref[1])))
    load = joined([-gu, gv])
    load_ref[...] = load
    send_ref[...] = joined([lane_blocks(-uv), packed(-uu), lane_blocks(load)])
    wl_ref[...] = wl
    back_ref[...] = joined([t2, t])


def on_owner(span, body):
    def kernel(slab_ref, *refs):
        @pl.when(lax.rem(slab_ref[0], span) == 0)
        def _():
            body(*refs)

    return kernel


def merge_kernel(theirs_ref, vv_ref, send_ref, w_ref, t_ref, new_vv_ref, buf):
    order = w_ref.shape[0]
    count = w_ref.shape[1] // LANES
    size = vv_ref.shape[0]
    unpack_to(buf.at[0], theirs_ref[...] + send_ref[count * order : count * order + size, :])
    w = invert(buf)[...]
    w_ref[...] = w
    second = from_lane_blocks(send_ref, 0, order, count)
    t = mm(second, embed(w))
    t_ref[...] = t
    new_vv_ref[...] = vv_ref[...] - packed(mm_t(t, embed(second)))


def side_kernel(w_ref, t_ref, mine_ref, theirs_ref, send_ref, load_ref, wl_ref, back_ref, st, rhs):
    order = w_ref.shape[0]
    count = w_ref.shape[1] // LANES
    rest = count * order
    cols = load_ref.shape[0] // 2
    size = send_ref.shape[0] - rest - count * 2 * cols
    second_e = embed(from_lane_blocks(mine_ref, 0, order, count))
    my_load = from_lane_blocks(mine_ref, rest + size, 2 * cols, count)
    their_load = from_lane_blocks(theirs_ref, rest + size, 2 * cols, count)
    t = t_ref[...]
    first_e = embed(from_lane_blocks(theirs_ref, 0, order, count))
    t2, wl, uv, uu, gu = side_products(w_ref[...], first_e, their_load[cols:] + my_load[:cols], t, st, rhs)
    gv = my_load[cols:] - mm_t(wl, second_e)
    load = joined([their_load[:cols] - gu, gv])
    load_ref[...] = load
    send_ref[...] = joined([lane_blocks(-uv), theirs_ref[rest : rest + size, :] - packed(uu), lane_blocks(load)])
    wl_ref[...] = wl
    back_ref[...] = joined([t2, t])


def edge_kernel(vv_ref, send_ref, load_ref, uu_ref, h_ref, y_ref, gu_ref, buf):
    order, count = buf.shape[1], buf.shape[2] // LANES
    cols = y_ref.shape[0]
    size = vv_ref.shape[0]
    unpack_to(buf.at[0], vv_ref[...])
    w = invert(buf)[...]
    second_e = embed(from_lane_blocks(send_ref, 0, order, count))
    own = mm(joined([first_rows(second_e.T), load_ref[cols:, :]]), embed(w))
    change = mm(own, second_e)
    uu_ref[...] = send_ref[count * order : count * order + size, :] - packed(change[:order])
    h_ref[...] = own[:order]
    y_ref[...] = own[order:]
    gu_ref[...] = load_ref[:cols, :] - change[order:]


def last_kernel(their_vv_ref, their_load_ref, uu_ref, h_ref, y_ref, gu_ref, out_ref, vl_ref, buf):
    cols = y_ref.shape[0]
    unpack_to(buf.at[0], their_vv_ref[...] + uu_ref[...])
    w = invert(buf)[...]
    mid = rows_times(their_load_ref[cols:, :] + gu_ref[...], w)
    out_ref[...] = joined([jnp.zeros_like(mid), mid])
    vl_ref[...] = y_ref[...] - rows_times(mid, h_ref[...])


def values_of(level, slab_ref, got_ref, prev_ref, vl_ref, wl_ref, back_ref):
    cols = wl_ref.shape[0]
    span = 2 << level
    aimed = lax.rem(slab_ref[0], span) == span // 2
    vu = jnp.where(aimed, got_ref[:cols, :], prev_ref[cols:, :])
    vl = jnp.where(aimed, got_ref[cols:, :], vl_ref[...])
    mid = wl_ref[...] - rows_times(jnp.concatenate([vu, vl], axis=1), back_ref[...])
    return vu, mid, vl


def back_kernel(level, slab_ref, got_ref, prev_ref, vl_ref, wl_ref, back_ref, out_ref, new_vl_ref):
    vu, mid, vl = values_of(level, slab_ref, got_ref, prev_ref, vl_ref, wl_ref, back_ref)
    out_ref[...] = joined([vu, mid])
    new_vl_ref[...] = vl


def end_kernel(slab_ref, got_ref, prev_ref, vl_ref, wl_ref, back_ref, out_ref):
    _, mid, vl = values_of(0, slab_ref, got_ref, prev_ref, vl_ref, wl_ref, back_ref)
    out_ref[0] = unblocked(vl)
    out_ref[1] = unblocked(mid)


def f32(*shape):
    return jax.ShapeDtypeStruct(shape, jnp.float32)


def run(kernel, outs, *args, scalars=0, flops=10**8, scratch=()):
    specs = [pl.BlockSpec(memory_space=pltpu.SMEM)] * scalars
    specs += [pl.BlockSpec(memory_space=pltpu.VMEM)] * (len(args) - scalars)
    return pl.pallas_call(
        kernel,
        out_shape=outs,
        in_specs=specs,
        out_specs=jax.tree.map(lambda _: pl.BlockSpec(memory_space=pltpu.VMEM), outs),
        scratch_shapes=list(scratch),
        compiler_params=pltpu.CompilerParams(vmem_limit_bytes=LIMIT),
        cost_estimate=pl.CostEstimate(flops=flops, bytes_accessed=10**6, transcendentals=0),
    )(*args)


def forward_to(x, axis, distance):
    n = lax.axis_size(axis)
    return lax.ppermute(x, axis, [(i + distance, i) for i in range(0, n, 2 * distance)])


def back_to(x, axis, distance):
    n = lax.axis_size(axis)
    return lax.ppermute(x, axis, [(i, i + distance) for i in range(0, n, 2 * distance)])


def gathered(diag_blocks):
    width = diag_blocks.shape[2]
    copies = [jnp.broadcast_to(layer, (lax.axis_size("orb"), *layer.shape)) for layer in diag_blocks]
    copies = jnp.where(lax.axis_index("rhs") == 0, copies[0], copies[1])
    whole = lax.all_to_all(copies, "orb", split_axis=0, concat_axis=0, tiled=True)
    return lax.all_gather(whole.reshape(-1, width), "rhs")


def local(diag_blocks, couplings, sources):
    order, width = couplings.shape[1:]
    cols = sources.shape[1]
    nb = order // HALF
    size = packed_rows(nb)
    whole = f32(order, width)
    vv_shape = f32(size, LANES)
    sides = (
        f32((order + 2 * cols) * width // LANES + size, LANES),
        f32(2 * cols, width),
        f32(cols, width),
        f32(2 * order, width),
    )
    slab = lax.axis_index("slab").astype(jnp.int32).reshape(1)
    heavy, light = 4 * 10**9, 10**9
    n = lax.axis_size("slab")
    following = lax.ppermute(couplings[0], "slab", [(i + 1, i) for i in range(n - 1)])
    levels = n.bit_length() - 1
    rhs = pltpu.VMEM((2, width, width), jnp.float32)
    buf = pltpu.VMEM((2, order, width), jnp.float32)
    for_pivot = (buf,)
    for_side = (pltpu.VMEM((5, order + cols, width), jnp.float32), rhs)
    pivots = (whole, whole, vv_shape)
    pair = f32(2 * cols, width)
    one = f32(cols, width)

    def on(level, kernel, outs, *args, flops, scratch):
        return run(on_owner(1 << level, kernel), outs, slab, *args, scalars=1, flops=flops, scratch=scratch)

    w, t, vv = run(start_kernel, pivots, gathered(diag_blocks), couplings, flops=heavy, scratch=for_pivot)
    stored = []
    for level in range(levels):
        their_vv = forward_to(vv, "slab", 1 << level)
        if level == 0:
            outs = run(
                start_side_kernel, sides, couplings, following, sources, w, t, flops=light, scratch=for_side
            )
        else:
            outs = on(level, side_kernel, sides, w, t, send, theirs, flops=light, scratch=for_side)
        send, load, wl, back = outs
        stored.append((wl, back))
        if level < levels - 1:
            theirs = forward_to(send, "slab", 1 << level)
            w, t, vv = on(
                level + 1, merge_kernel, pivots, their_vv, vv, send, flops=heavy, scratch=for_pivot
            )
    theirs = forward_to(load, "slab", 1 << (levels - 1))
    edge = on(
        levels, edge_kernel, (vv_shape, whole, one, one), vv, send, load, flops=heavy, scratch=for_pivot
    )
    values, vl = on(
        levels, last_kernel, (pair, one), their_vv, theirs, *edge, flops=heavy, scratch=for_pivot
    )
    for level in reversed(range(levels)):
        got = back_to(values, "slab", 1 << level)
        wl, back = stored[level]
        if level > 0:
            values, vl = run(
                functools.partial(back_kernel, level),
                (pair, one),
                slab, got, values, vl, wl, back,
                scalars=1, flops=10**7,
            )
    return run(end_kernel, f32(2, cols, width), slab, got, values, vl, wl, back, scalars=1, flops=10**7)


def solution(mesh):
    placed = (
        P(("energy", "slab"), "orb", None),
        P(("energy", "slab"), None, None),
        P(("energy", "slab"), ("orb", "rhs"), None),
    )
    return jax.shard_map(
        local,
        mesh=mesh,
        in_specs=placed,
        out_specs=P(("energy", "slab"), ("orb", "rhs"), None),
        check_vma=False,
    )
```

```python
import functools
import jax
import jax.numpy as jnp
from jax import lax
from jax.experimental import pallas as pl
from jax.experimental.pallas import tpu as pltpu
from jax.sharding import PartitionSpec as P


HI = lax.Precision.HIGHEST
LANES = 128
HALF = 64
SUB = 8
LIMIT = 16 * 2**20


def mm(a, b):
    return lax.dot_general(a, b, (((1,), (0,)), ((), ())), precision=HI, preferred_element_type=jnp.float32)


def mm_t(a, b):
    return lax.dot_general(a, b, (((1,), (1,)), ((), ())), precision=HI, preferred_element_type=jnp.float32)


def lanes_of(x):
    return lax.broadcasted_iota(jnp.int32, x.shape, 1)


def times_i(x):
    parts = []
    for b in range(x.shape[1] // LANES):
        blk = x[:, b * LANES : (b + 1) * LANES]
        rolled = pltpu.roll(blk, HALF, 1)
        parts.append(jnp.where(lanes_of(blk) < HALF, -rolled, rolled))
    return jnp.concatenate(parts, axis=1)


def embed(z):
    rows = []
    turned = times_i(z)
    for a in range(z.shape[0] // HALF):
        rows.append(z[a * HALF : (a + 1) * HALF])
        rows.append(turned[a * HALF : (a + 1) * HALF])
    return jnp.concatenate(rows, axis=0)


def first_rows(e):
    return jnp.concatenate([e[a * LANES : a * LANES + HALF] for a in range(e.shape[0] // LANES)], axis=0)


def blocked(x):
    v0, v1, v2 = (x[:, LANES * b : LANES * (b + 1)] for b in range(3))
    low = lanes_of(v0) < HALF
    return jnp.concatenate(
        [jnp.where(low, v0, v1), pltpu.roll(jnp.where(low, v2, v0), HALF, 1), jnp.where(low, v1, v2)], axis=1
    )


def unblocked(x):
    u0, u1, u2 = (x[:, LANES * b : LANES * (b + 1)] for b in range(3))
    low = lanes_of(u0) < HALF
    r1 = pltpu.roll(u1, HALF, 1)
    return jnp.concatenate([jnp.where(low, u0, r1), jnp.where(low, u2, u0), jnp.where(low, r1, u2)], axis=1)


def pairs(n):
    return [(a, b) for a in range(n) for b in range(a + 1, n)]


def packed_rows(n):
    return len(pairs(n)) * HALF + n // 2 * HALF + n % 2 * (HALF // 2)


def halves_of(block):
    low = lanes_of(block) < HALF
    row = lax.broadcasted_iota(jnp.int32, block.shape, 0)
    col = jnp.where(low, lanes_of(block), lanes_of(block) - HALF)
    return low, row, col


def hermitian_low(block):
    _, row, col = halves_of(block)
    return jnp.where(row <= col, block, pltpu.roll(block, HALF, 1))


def hermitian_high(block):
    _, row, col = halves_of(block)
    return jnp.where(row <= col, pltpu.roll(block, HALF, 1), block)


def packed(z):
    n = z.shape[0] // HALF

    def block(a, b):
        return z[a * HALF : (a + 1) * HALF, b * LANES : (b + 1) * LANES]

    parts = [block(a, b) for a, b in pairs(n)]
    for a in range(0, n - 1, 2):
        first, second = hermitian_low(block(a, a)), hermitian_high(block(a + 1, a + 1))
        parts.append(jnp.where(lanes_of(first) < HALF, first, second))
    if n % 2:
        last = hermitian_low(block(n - 1, n - 1))
        top, bottom = last[: HALF // 2], pltpu.roll(last[HALF // 2 :], HALF, 1)
        parts.append(jnp.where(lanes_of(top) < HALF, top, bottom))
    return jnp.concatenate(parts, axis=0)


def hermitian(half):
    low, row, col = halves_of(half)
    twice = jnp.where(low, half, pltpu.roll(half, HALF, 1))
    t = twice.T
    flipped = jnp.concatenate([t[:HALF], t[HALF:]], axis=1)
    re = jnp.where(row <= col, twice, flipped)
    im = jnp.where(row > col, twice, jnp.where(row < col, -flipped, 0.0))
    return jnp.where(low, re, im)


def adjoint(block):
    t = block.T
    return jnp.concatenate([t[:HALF], -t[HALF:]], axis=1)


def unpack_to(ref, p):
    n = ref.shape[0] // HALF

    def put(a, b, block):
        ref[a * HALF : (a + 1) * HALF, b * LANES : (b + 1) * LANES] = block

    for k, (a, b) in enumerate(pairs(n)):
        block = p[k * HALF : (k + 1) * HALF]
        put(a, b, block)
        put(b, a, adjoint(block))
    start = len(pairs(n)) * HALF
    for a in range(0, n - 1, 2):
        block = p[start : start + HALF]
        put(a, a, hermitian(block))
        put(a + 1, a + 1, hermitian(pltpu.roll(block, HALF, 1)))
        start += HALF
    if n % 2:
        block = p[start : start + HALF // 2]
        put(n - 1, n - 1, hermitian(jnp.concatenate([block, pltpu.roll(block, HALF, 1)], axis=0)))


def lane_copy(x, lane):
    return jnp.broadcast_to(x[:, lane : lane + 1], (SUB, LANES))


def row_copy(x, row):
    return jnp.broadcast_to(x[row : row + 1, :], (SUB, LANES))


def invert(buf):
    nb = buf.shape[1] // HALF
    groups = HALF // SUB
    lane = lax.broadcasted_iota(jnp.int32, (SUB, LANES), 1)
    sub = lax.broadcasted_iota(jnp.int32, (SUB, LANES), 0)
    low = lane < HALF
    lane_in = jnp.where(low, lane, lane - HALF)

    def at(a, b):
        return (slice(a * HALF, (a + 1) * HALF), slice(b * LANES, (b + 1) * LANES))

    def step(i, carry):
        cur, nxt = buf.at[lax.rem(i, 2)], buf.at[lax.rem(i + 1, 2)]
        x = [cur[g * SUB : (g + 1) * SUB, :LANES] for g in range(groups)]
        for t in range(groups):
            z = x[t]
            y = times_i(z)
            vr = [lane_copy(z, SUB * t + j) for j in range(SUB)]
            vi = [lane_copy(z, HALF + SUB * t + j) for j in range(SUB)]
            for p in range(SUB):
                here = sub == p
                col = lane_in == SUB * t + p
                rinv = 1.0 / row_copy(vr[p], p)
                fr = jnp.where(here, 1.0 - rinv, vr[p] * rinv)
                fi = jnp.where(here, 0.0, vi[p] * rinv)
                for j in range(p + 1, SUB):
                    ar, ai = row_copy(vr[j], p), row_copy(vi[j], p)
                    vr[j] = vr[j] - (fr * ar - fi * ai)
                    vi[j] = vi[j] - (fr * ai + fi * ar)
                unit = jnp.where(here, 1.0, 0.0)
                z = jnp.where(col, jnp.where(low, unit, 0.0), z)
                y = jnp.where(col, jnp.where(low, 0.0, unit), y)
                zr, yr = row_copy(z, p), row_copy(y, p)
                z, y = z - (fr * zr + fi * yr), y - (fr * yr - fi * zr)
            x[t] = z
            zs = [row_copy(z, j) for j in range(SUB)]
            ys = [row_copy(y, j) for j in range(SUB)]
            cols = (lane_in >= SUB * t) & (lane_in < SUB * (t + 1))
            for g in [(t + 1 + s) % groups for s in range(groups - 1)]:
                acc = [
                    lane_copy(x[g], SUB * t + j) * zs[j] + lane_copy(x[g], HALF + SUB * t + j) * ys[j]
                    for j in range(SUB)
                ]
                while len(acc) > 1:
                    acc = [acc[q] + acc[q + 1] for q in range(0, len(acc), 2)]
                x[g] = jnp.where(cols, 0.0, x[g]) - acc[0]
        d = jnp.concatenate(x, axis=0)
        rest = cur[:HALF, LANES:]
        rest = mm(d, jnp.concatenate([rest, times_i(rest)], axis=0))
        zp = jnp.concatenate([d, rest], axis=1)
        for b in range(nb):
            nxt[at(nb - 1, (b - 1) % nb)] = zp[:, b * LANES : (b + 1) * LANES]
        change = mm(cur[HALF:, :LANES], jnp.concatenate([zp, times_i(zp)], axis=0))
        for a in range(1, nb):
            for b in range(nb):
                piece = change[(a - 1) * HALF : a * HALF, b * LANES : (b + 1) * LANES]
                nxt[at(a - 1, (b - 1) % nb)] = -piece if b == 0 else cur[at(a, b)] - piece
        return carry

    lax.fori_loop(0, nb, step, 0)
    return buf.at[nb % 2]


def rows_times(x, z):
    blocks = [x[:, b * LANES : (b + 1) * LANES] for b in range(x.shape[1] // LANES)]
    low = lanes_of(blocks[0]) < HALF
    turned = [pltpu.roll(b, HALF, 1) for b in blocks]
    even = range(0, len(blocks) - 1, 2)
    re = [jnp.where(low, blocks[b], turned[b + 1]) for b in even]
    im = [jnp.where(low, turned[b], blocks[b + 1]) for b in even]
    if len(blocks) % 2:
        re.append(blocks[-1][:, :HALF])
        im.append(turned[-1][:, :HALF])
    both = jnp.concatenate([jnp.concatenate(re, axis=1), jnp.concatenate(im, axis=1)], axis=0)
    got = mm(both, z)
    n = x.shape[0]
    return got[:n] + times_i(got[n:])


def joined(blocks):
    return jnp.concatenate(blocks, axis=0)


def lane_blocks(z):
    return joined([z[:, b * LANES : (b + 1) * LANES] for b in range(z.shape[1] // LANES)])


def from_lane_blocks(ref, start, rows, count):
    return jnp.concatenate([ref[start + b * rows : start + (b + 1) * rows, :] for b in range(count)], axis=1)


def chained(st, rhs, steps):
    def step(i, carry):
        frm, to, which = steps(i)
        st[to] = mm(st[frm], rhs[which])
        return carry

    return step


def start_kernel(diag_ref, coup_ref, w_ref, t_ref, vv_ref, buf):
    buf[0] = blocked(diag_ref[1])
    w = invert(buf)[...]
    w_ref[...] = w
    second = blocked(coup_ref[1])
    t = mm(second, embed(w))
    t_ref[...] = t
    vv_ref[...] = packed(blocked(diag_ref[0]) - mm_t(t, embed(second)))


def side_products(w, first_e, loads, t, st, rhs):
    order = w.shape[0]
    rhs[0] = embed(w)
    rhs[1] = first_e
    st[0, :order] = first_rows(first_e.T)
    st[0, order:] = loads
    st[2, :order] = t
    st[2, order:] = jnp.zeros_like(loads)
    lax.fori_loop(0, 3, chained(st, rhs, lambda i: (i, i + 1 + jnp.minimum(i, 1), jnp.minimum(i, 1))), 0)
    return st[1, :order], st[1, order:], st[4, :order], st[3, :order], st[3, order:]


def start_side_kernel(coup_ref, next_ref, src_ref, w_ref, t_ref, send_ref, load_ref, wl_ref, back_ref, st, rhs):
    t = t_ref[...]
    first_e = embed(blocked(next_ref[...]))
    t2, wl, uv, uu, gu = side_products(w_ref[...], first_e, blocked(src_ref[1]), t, st, rhs)
    gv = blocked(src_ref[0]) - mm_t(wl, embed(blocked(coup_ref[1])))
    load = joined([-gu, gv])
    load_ref[...] = load
    send_ref[...] = joined([lane_blocks(-uv), packed(-uu), lane_blocks(load)])
    wl_ref[...] = wl
    back_ref[...] = joined([t2, t])


def on_owner(span, body):
    def kernel(slab_ref, *refs):
        @pl.when(lax.rem(slab_ref[0], span) == 0)
        def _():
            body(*refs)

    return kernel


def merge_kernel(theirs_ref, vv_ref, send_ref, w_ref, t_ref, new_vv_ref, buf):
    order = w_ref.shape[0]
    count = w_ref.shape[1] // LANES
    size = vv_ref.shape[0]
    unpack_to(buf.at[0], theirs_ref[...] + send_ref[count * order : count * order + size, :])
    w = invert(buf)[...]
    w_ref[...] = w
    second = from_lane_blocks(send_ref, 0, order, count)
    t = mm(second, embed(w))
    t_ref[...] = t
    new_vv_ref[...] = vv_ref[...] - packed(mm_t(t, embed(second)))


def side_kernel(w_ref, t_ref, mine_ref, theirs_ref, send_ref, load_ref, wl_ref, back_ref, st, rhs):
    order = w_ref.shape[0]
    count = w_ref.shape[1] // LANES
    rest = count * order
    cols = load_ref.shape[0] // 2
    size = send_ref.shape[0] - rest - count * 2 * cols
    second_e = embed(from_lane_blocks(mine_ref, 0, order, count))
    my_load = from_lane_blocks(mine_ref, rest + size, 2 * cols, count)
    their_load = from_lane_blocks(theirs_ref, rest + size, 2 * cols, count)
    t = t_ref[...]
    first_e = embed(from_lane_blocks(theirs_ref, 0, order, count))
    t2, wl, uv, uu, gu = side_products(w_ref[...], first_e, their_load[cols:] + my_load[:cols], t, st, rhs)
    gv = my_load[cols:] - mm_t(wl, second_e)
    load = joined([their_load[:cols] - gu, gv])
    load_ref[...] = load
    send_ref[...] = joined([lane_blocks(-uv), theirs_ref[rest : rest + size, :] - packed(uu), lane_blocks(load)])
    wl_ref[...] = wl
    back_ref[...] = joined([t2, t])


def edge_kernel(vv_ref, send_ref, load_ref, uu_ref, h_ref, y_ref, gu_ref, buf):
    order, count = buf.shape[1], buf.shape[2] // LANES
    cols = y_ref.shape[0]
    size = vv_ref.shape[0]
    unpack_to(buf.at[0], vv_ref[...])
    w = invert(buf)[...]
    second_e = embed(from_lane_blocks(send_ref, 0, order, count))
    own = mm(joined([first_rows(second_e.T), load_ref[cols:, :]]), embed(w))
    change = mm(own, second_e)
    uu_ref[...] = send_ref[count * order : count * order + size, :] - packed(change[:order])
    h_ref[...] = own[:order]
    y_ref[...] = own[order:]
    gu_ref[...] = load_ref[:cols, :] - change[order:]


def last_kernel(their_vv_ref, their_load_ref, uu_ref, h_ref, y_ref, gu_ref, out_ref, vl_ref, buf):
    cols = y_ref.shape[0]
    unpack_to(buf.at[0], their_vv_ref[...] + uu_ref[...])
    w = invert(buf)[...]
    mid = rows_times(their_load_ref[cols:, :] + gu_ref[...], w)
    out_ref[...] = joined([jnp.zeros_like(mid), mid])
    vl_ref[...] = y_ref[...] - rows_times(mid, h_ref[...])


def values_of(level, slab_ref, got_ref, prev_ref, vl_ref, wl_ref, back_ref):
    cols = wl_ref.shape[0]
    span = 2 << level
    aimed = lax.rem(slab_ref[0], span) == span // 2
    vu = jnp.where(aimed, got_ref[:cols, :], prev_ref[cols:, :])
    vl = jnp.where(aimed, got_ref[cols:, :], vl_ref[...])
    mid = wl_ref[...] - rows_times(jnp.concatenate([vu, vl], axis=1), back_ref[...])
    return vu, mid, vl


def back_kernel(level, slab_ref, got_ref, prev_ref, vl_ref, wl_ref, back_ref, out_ref, new_vl_ref):
    vu, mid, vl = values_of(level, slab_ref, got_ref, prev_ref, vl_ref, wl_ref, back_ref)
    out_ref[...] = joined([vu, mid])
    new_vl_ref[...] = vl


def end_kernel(slab_ref, got_ref, prev_ref, vl_ref, wl_ref, back_ref, out_ref):
    _, mid, vl = values_of(0, slab_ref, got_ref, prev_ref, vl_ref, wl_ref, back_ref)
    out_ref[0] = unblocked(vl)
    out_ref[1] = unblocked(mid)


def f32(*shape):
    return jax.ShapeDtypeStruct(shape, jnp.float32)


def run(kernel, outs, *args, scalars=0, flops=10**8, scratch=()):
    specs = [pl.BlockSpec(memory_space=pltpu.SMEM)] * scalars
    specs += [pl.BlockSpec(memory_space=pltpu.VMEM)] * (len(args) - scalars)
    return pl.pallas_call(
        kernel,
        out_shape=outs,
        in_specs=specs,
        out_specs=jax.tree.map(lambda _: pl.BlockSpec(memory_space=pltpu.VMEM), outs),
        scratch_shapes=list(scratch),
        compiler_params=pltpu.CompilerParams(vmem_limit_bytes=LIMIT),
        cost_estimate=pl.CostEstimate(flops=flops, bytes_accessed=10**6, transcendentals=0),
    )(*args)


def forward_to(x, axis, distance):
    n = lax.axis_size(axis)
    return lax.ppermute(x, axis, [(i + distance, i) for i in range(0, n, 2 * distance)])


def back_to(x, axis, distance):
    n = lax.axis_size(axis)
    return lax.ppermute(x, axis, [(i, i + distance) for i in range(0, n, 2 * distance)])


def copies_kernel(which_ref, diag_ref, out_ref):
    mine = jnp.where(which_ref[0] == 0, diag_ref[0], diag_ref[1])
    for k in range(out_ref.shape[0]):
        out_ref[k] = mine


def gathered(diag_blocks):
    which = lax.axis_index("rhs").astype(jnp.int32).reshape(1)
    shape = (lax.axis_size("orb"), *diag_blocks.shape[1:])
    copies = run(copies_kernel, f32(*shape), which, diag_blocks, scalars=1, flops=10**6)
    whole = lax.all_to_all(copies, "orb", split_axis=0, concat_axis=0, tiled=True)
    return lax.all_gather(whole.reshape(-1, shape[2]), "rhs")


def local(diag_blocks, couplings, sources):
    order, width = couplings.shape[1:]
    cols = sources.shape[1]
    nb = order // HALF
    size = packed_rows(nb)
    whole = f32(order, width)
    vv_shape = f32(size, LANES)
    sides = (
        f32((order + 2 * cols) * width // LANES + size, LANES),
        f32(2 * cols, width),
        f32(cols, width),
        f32(2 * order, width),
    )
    slab = lax.axis_index("slab").astype(jnp.int32).reshape(1)
    heavy, light = 4 * 10**9, 10**9
    n = lax.axis_size("slab")
    following = lax.ppermute(couplings[0], "slab", [(i + 1, i) for i in range(n - 1)])
    levels = n.bit_length() - 1
    rhs = pltpu.VMEM((2, width, width), jnp.float32)
    buf = pltpu.VMEM((2, order, width), jnp.float32)
    for_pivot = (buf,)
    for_side = (pltpu.VMEM((5, order + cols, width), jnp.float32), rhs)
    pivots = (whole, whole, vv_shape)
    pair = f32(2 * cols, width)
    one = f32(cols, width)

    def on(level, kernel, outs, *args, flops, scratch):
        return run(on_owner(1 << level, kernel), outs, slab, *args, scalars=1, flops=flops, scratch=scratch)

    w, t, vv = run(start_kernel, pivots, gathered(diag_blocks), couplings, flops=heavy, scratch=for_pivot)
    stored = []
    for level in range(levels):
        their_vv = forward_to(vv, "slab", 1 << level)
        if level == 0:
            outs = run(
                start_side_kernel, sides, couplings, following, sources, w, t, flops=light, scratch=for_side
            )
        else:
            outs = on(level, side_kernel, sides, w, t, send, theirs, flops=light, scratch=for_side)
        send, load, wl, back = outs
        stored.append((wl, back))
        if level < levels - 1:
            theirs = forward_to(send, "slab", 1 << level)
            w, t, vv = on(
                level + 1, merge_kernel, pivots, their_vv, vv, send, flops=heavy, scratch=for_pivot
            )
    theirs = forward_to(load, "slab", 1 << (levels - 1))
    edge = on(
        levels, edge_kernel, (vv_shape, whole, one, one), vv, send, load, flops=heavy, scratch=for_pivot
    )
    values, vl = on(
        levels, last_kernel, (pair, one), their_vv, theirs, *edge, flops=heavy, scratch=for_pivot
    )
    for level in reversed(range(levels)):
        got = back_to(values, "slab", 1 << level)
        wl, back = stored[level]
        if level > 0:
            values, vl = run(
                functools.partial(back_kernel, level),
                (pair, one),
                slab, got, values, vl, wl, back,
                scalars=1, flops=10**7,
            )
    return run(end_kernel, f32(2, cols, width), slab, got, values, vl, wl, back, scalars=1, flops=10**7)


def solution(mesh):
    placed = (
        P(("energy", "slab"), "orb", None),
        P(("energy", "slab"), None, None),
        P(("energy", "slab"), ("orb", "rhs"), None),
    )
    return jax.shard_map(
        local,
        mesh=mesh,
        in_specs=placed,
        out_specs=P(("energy", "slab"), ("orb", "rhs"), None),
        check_vma=False,
    )
```
